32 devices in a mesh: dp: 1 (over z), ep: 32 (over y, x, core).
Axes of the slice: x: 4, y: 4, z: 1, core: 2. Of those that a mesh axis runs over, the one named last changes fastest.
The devices are a block of a 4x4x8 slice.
Arguments:
- grad_out: bfloat16 [2, 8192, 1024], P(None, ('dp', 'ep'))
- expert_out: bfloat16 [2, 8192, 8, 1024], P(None, ('dp', 'ep'))
- gate_vals: float32 [2, 8192, 8], P(None, ('dp', 'ep'))
- topk_idx: int32 [2, 8192, 8], P(None, ('dp', 'ep'))
- slot_idx: int32 [2, 8192, 8], P(None, ('dp', 'ep'))
- x_dispatch: bfloat16 [2, 32, 2816, 1024], P(None, ('dp', 'ep'))
- h1_pre: bfloat16 [2, 32, 2816, 512], P(None, ('dp', 'ep'))
- h3_pre: bfloat16 [2, 32, 2816, 512], P(None, ('dp', 'ep'))
- w_gate: bfloat16 [32, 1024, 512], P('ep')
- w_up: bfloat16 [32, 1024, 512], P('ep')
- w_down: bfloat16 [32, 512, 1024], P('ep')
Outputs:
- output 1: bfloat16 [2, 8192, 1024], P(None, ('dp', 'ep'))
- output 2: float32 [2, 8192, 8], P(None, ('dp', 'ep'))
- output 3: float32 [32, 1024, 512], P(('dp', 'ep'))
- output 4: float32 [32, 1024, 512], P(('dp', 'ep'))
- output 5: float32 [32, 512, 1024], P(('dp', 'ep'))
All inputs are finite; a program needn't handle non-finite values.
Results may differ from the reference program's by a relative error of at most 0.0116613.
Values are sent between devices in bfloat16 or wider.
A program may use at most 768 MiB of HBM per device.

```python
import jax
import jax.numpy as jnp
from jax import lax

GROUP_SIZE = 32
TOKENS = 256
EXPERTS = 32
TOP_K = 8
D_MODEL = 1024
D_FF = 512
MICRO_BATCHES = 2
CAPACITY = 8 * ((5 * TOKENS * TOP_K) // (32 * EXPERTS) + 1)
BUF_ROWS = GROUP_SIZE * CAPACITY
GROUP_TOKENS = GROUP_SIZE * TOKENS
TOTAL_ROWS = EXPERTS * BUF_ROWS


def route_tokens(rng_key):
    key_base, key_bias, key_hot = jax.random.split(rng_key, 3)
    base_score = jax.random.randint(key_base, (GROUP_SIZE, TOKENS, EXPERTS), 0, 1024)
    expert_bias = jax.random.randint(key_bias, (EXPERTS,), 0, 1024)
    hot_expert = jax.random.randint(key_hot, (GROUP_SIZE, 1, 1), 0, EXPERTS)
    expert_ids = jnp.arange(EXPERTS)
    forced = jnp.where((jnp.arange(TOKENS)[None, :, None] <= CAPACITY) & (expert_ids[None, None, :] == hot_expert), 4096, 0)
    score_int = (base_score + expert_bias + forced) * EXPERTS + expert_ids
    topk_idx = lax.top_k(score_int, TOP_K)[1].astype(jnp.int32)
    flat_choice = topk_idx.reshape(GROUP_SIZE, TOKENS * TOP_K)
    onehot = (flat_choice[:, :, None] == expert_ids).astype(jnp.int32)
    count_before = jnp.cumsum(onehot, axis=1) - onehot
    position = jnp.sum(count_before * onehot, axis=2).reshape(GROUP_SIZE, TOKENS, TOP_K)
    slot_idx = jnp.where(position < CAPACITY, position, -1).astype(jnp.int32)
    return topk_idx.reshape(GROUP_TOKENS, TOP_K), slot_idx.reshape(GROUP_TOKENS, TOP_K)


def buffer_rows(topk_idx, slot_idx):
    source = (jnp.arange(GROUP_TOKENS) // TOKENS)[:, None]
    flat_row = (topk_idx * GROUP_SIZE + source) * CAPACITY + slot_idx
    return jnp.where(slot_idx >= 0, flat_row, TOTAL_ROWS)


def scatter_rows(flat_row, values):
    row_width = values.shape[-1]
    buffer = jnp.zeros((TOTAL_ROWS + 1, row_width), jnp.bfloat16)
    buffer = buffer.at[flat_row.reshape(-1)].set(values.reshape(-1, row_width))
    return buffer[:TOTAL_ROWS].reshape(EXPERTS, BUF_ROWS, row_width)


def gather_rows(expert_rows, flat_row):
    row_width = expert_rows.shape[-1]
    padded = jnp.concatenate([expert_rows.reshape(TOTAL_ROWS, row_width), jnp.zeros((1, row_width), expert_rows.dtype)], axis=0)
    return padded[flat_row]


def expert_forward(operands):
    x_rows, w_gate_e, w_up_e, w_down_e = operands
    x_f32 = x_rows.astype(jnp.float32)
    h1_rows = jnp.einsum('mrd,df->mrf', x_f32, w_gate_e.astype(jnp.float32)).astype(jnp.bfloat16)
    h3_rows = jnp.einsum('mrd,df->mrf', x_f32, w_up_e.astype(jnp.float32)).astype(jnp.bfloat16)
    h1_f32 = h1_rows.astype(jnp.float32)
    activation = (h1_f32 * jax.nn.sigmoid(h1_f32) * h3_rows.astype(jnp.float32)).astype(jnp.bfloat16)
    y_rows = jnp.einsum('mrf,fd->mrd', activation.astype(jnp.float32), w_down_e.astype(jnp.float32)).astype(jnp.bfloat16)
    return h1_rows, h3_rows, y_rows


def saved_forward(x_home, topk_idx, slot_idx, w_gate, w_up, w_down):
    flat_row = jax.vmap(buffer_rows)(topk_idx, slot_idx)
    x_rep = jnp.broadcast_to(x_home[:, :, None, :], (MICRO_BATCHES, GROUP_TOKENS, TOP_K, D_MODEL))
    x_dispatch = jax.vmap(scatter_rows)(flat_row, x_rep)
    h1_e, h3_e, y_e = lax.map(expert_forward, (jnp.moveaxis(x_dispatch, 1, 0), w_gate, w_up, w_down))
    expert_out = jax.vmap(gather_rows)(jnp.moveaxis(y_e, 0, 1), flat_row)
    return x_dispatch, jnp.moveaxis(h1_e, 0, 1), jnp.moveaxis(h3_e, 0, 1), expert_out


def setup_inputs(seed: int = 0, part: int = 0) -> dict:
    root_key = jax.random.key(seed)
    key_shared, key_parts = jax.random.split(root_key)
    key_wg, key_wu, key_wd = jax.random.split(key_shared, 3)
    w_gate = (jax.random.normal(key_wg, (EXPERTS, D_MODEL, D_FF), jnp.float32) * D_MODEL ** -0.5).astype(jnp.bfloat16)
    w_up = (jax.random.normal(key_wu, (EXPERTS, D_MODEL, D_FF), jnp.float32) * D_MODEL ** -0.5).astype(jnp.bfloat16)
    w_down = (jax.random.normal(key_wd, (EXPERTS, D_FF, D_MODEL), jnp.float32) * D_FF ** -0.5).astype(jnp.bfloat16)
    key_part = jax.random.fold_in(key_parts, part)
    key_route, key_x, key_dy, key_gate = jax.random.split(key_part, 4)
    topk_idx, slot_idx = jax.vmap(route_tokens)(jax.random.split(key_route, MICRO_BATCHES))
    x_home = jax.random.normal(key_x, (MICRO_BATCHES, GROUP_TOKENS, D_MODEL), jnp.float32).astype(jnp.bfloat16)
    grad_out = jax.random.normal(key_dy, (MICRO_BATCHES, GROUP_TOKENS, D_MODEL), jnp.float32).astype(jnp.bfloat16)
    gate_vals = jax.random.uniform(key_gate, (MICRO_BATCHES, GROUP_TOKENS, TOP_K), jnp.float32, 0.25, 1.0)
    x_dispatch, h1_pre, h3_pre, expert_out = saved_forward(x_home, topk_idx, slot_idx, w_gate, w_up, w_down)
    return {'grad_out': grad_out, 'expert_out': expert_out, 'gate_vals': gate_vals, 'topk_idx': topk_idx, 'slot_idx': slot_idx, 'x_dispatch': x_dispatch, 'h1_pre': h1_pre, 'h3_pre': h3_pre, 'w_gate': w_gate, 'w_up': w_up, 'w_down': w_down}


def gate_grad(operands):
    dy_block, y_block = operands
    return jnp.einsum('td,tkd->tk', dy_block.astype(jnp.float32), y_block.astype(jnp.float32))


def expert_backward(operands):
    x_rows, h1_rows, h3_rows, dy_rows, w_gate_e, w_up_e, w_down_e = operands
    h1_f32 = h1_rows.astype(jnp.float32)
    h3_f32 = h3_rows.astype(jnp.float32)
    sigmoid_h1 = jax.nn.sigmoid(h1_f32)
    silu_h1 = h1_f32 * sigmoid_h1
    activation = (silu_h1 * h3_f32).astype(jnp.bfloat16)
    dy_f32 = dy_rows.astype(jnp.float32)
    x_f32 = x_rows.astype(jnp.float32)
    grad_act = jnp.einsum('mrd,fd->mrf', dy_f32, w_down_e.astype(jnp.float32)).astype(jnp.bfloat16).astype(jnp.float32)
    grad_h1 = (grad_act * h3_f32 * sigmoid_h1 * (1.0 + h1_f32 * (1.0 - sigmoid_h1))).astype(jnp.bfloat16)
    grad_h3 = (grad_act * silu_h1).astype(jnp.bfloat16)
    g_down = jnp.einsum('mrf,mrd->fd', activation.astype(jnp.float32), dy_f32)
    g_gate = jnp.einsum('mrd,mrf->df', x_f32, grad_h1.astype(jnp.float32))
    g_up = jnp.einsum('mrd,mrf->df', x_f32, grad_h3.astype(jnp.float32))
    dx_rows = (jnp.einsum('mrf,df->mrd', grad_h1.astype(jnp.float32), w_gate_e.astype(jnp.float32)) + jnp.einsum('mrf,df->mrd', grad_h3.astype(jnp.float32), w_up_e.astype(jnp.float32))).astype(jnp.bfloat16)
    return g_gate, g_up, g_down, dx_rows


def reference(grad_out, expert_out, gate_vals, topk_idx, slot_idx, x_dispatch, h1_pre, h3_pre, w_gate, w_up, w_down):
    blocks = MICRO_BATCHES * GROUP_SIZE
    grad_gate = lax.map(gate_grad, (grad_out.reshape(blocks, TOKENS, D_MODEL), expert_out.reshape(blocks, TOKENS, TOP_K, D_MODEL)))
    grad_gate = grad_gate.reshape(MICRO_BATCHES, GROUP_TOKENS, TOP_K)
    flat_row = jax.vmap(buffer_rows)(topk_idx, slot_idx)
    gated_rows = (gate_vals[:, :, :, None] * grad_out[:, :, None, :].astype(jnp.float32)).astype(jnp.bfloat16)
    dy_dispatch = jax.vmap(scatter_rows)(flat_row, gated_rows)
    grad_w_gate, grad_w_up, grad_w_down, dx_rows = lax.map(expert_backward, (jnp.moveaxis(x_dispatch, 1, 0), jnp.moveaxis(h1_pre, 1, 0), jnp.moveaxis(h3_pre, 1, 0), jnp.moveaxis(dy_dispatch, 1, 0), w_gate, w_up, w_down))
    returned = jax.vmap(gather_rows)(jnp.moveaxis(dx_rows, 0, 1), flat_row)
    grad_x = jnp.sum(returned.astype(jnp.float32), axis=2).astype(jnp.bfloat16)
    return (grad_x, grad_gate, grad_w_gate, grad_w_up, grad_w_down)
```

```python
import functools
import jax
import jax.numpy as jnp
from jax import lax
from jax.experimental import pallas as pl
from jax.experimental.pallas import tpu as pltpu
from jax.sharding import PartitionSpec as P

F32 = jnp.float32
BF16 = jnp.bfloat16


def dot_nn(a, b):
    return lax.dot_general(a, b, (((1,), (0,)), ((), ())), preferred_element_type=F32)


def dot_nt(a, b):
    return lax.dot_general(a, b, (((1,), (1,)), ((), ())), preferred_element_type=F32)


def dot_tn(a, b):
    return lax.dot_general(a, b, (((0,), (0,)), ((), ())), preferred_element_type=F32)


def gather_rows(pos, gate, dy, rows):
    tokens = pos.shape[1]
    hit = lax.broadcasted_iota(jnp.int32, (rows, tokens), 0).astype(F32) == pos
    gate_col = jnp.sum(jnp.where(hit, gate, 0.0), axis=1, keepdims=True)
    onehot = jnp.where(hit, 1.0, 0.0).astype(BF16)
    return (dot_nn(onehot, dy) * gate_col).astype(BF16)


def swiglu_grads(dyd, h1, h3, w2):
    h1 = h1.astype(F32)
    h3 = h3.astype(F32)
    sig = jax.nn.sigmoid(h1)
    silu = h1 * sig
    act = (silu * h3).astype(BF16)
    da = dot_nt(dyd, w2).astype(BF16).astype(F32)
    dh1 = (da * h3 * sig * (1.0 + h1 * (1.0 - sig))).astype(BF16)
    dh3 = (da * silu).astype(BF16)
    return act, dh1, dh3


def expert_kernel(first, pos, gate, dy, x, h1, h3, w1, w3, w2, *refs):
    if first:
        dx, g1, g3, g2 = refs
    else:
        p1, p3, p2, dx, g1, g3, g2 = refs
    rows = x.shape[0]
    dyd = gather_rows(pos[0], gate[0], dy[0], rows)
    act, dh1, dh3 = swiglu_grads(dyd, h1[...], h3[...], w2[...])
    dx[...] = (dot_nt(dh1, w1[...]) + dot_nt(dh3, w3[...])).astype(BF16)

    @pl.when(pl.program_id(0) == 0)
    def _():
        for k, g in enumerate((g1, g3, g2)):
            g[...] = jnp.zeros_like(g) if first else (p1, p3, p2)[k][...]

    g1[...] += dot_tn(x[...], dh1)
    g3[...] += dot_tn(x[...], dh3)
    g2[...] += dot_tn(act, dyd)


def expert_call(pos, gate, dy, x, h1, h3, w1, w3, w2, prev):
    units, tokens, d = dy.shape
    f = h1.shape[1]
    rows = x.shape[0] // units
    whole = lambda a, b: pl.BlockSpec((a, b), lambda i: (0, 0))
    in_specs = [pl.BlockSpec((1, 1, tokens), lambda i: (i, 0, 0))] * 2 + [
        pl.BlockSpec((1, tokens, d), lambda i: (i, 0, 0)),
        pl.BlockSpec((rows, d), lambda i: (i, 0)),
        pl.BlockSpec((rows, f), lambda i: (i, 0)),
        pl.BlockSpec((rows, f), lambda i: (i, 0)),
        whole(d, f), whole(d, f), whole(f, d)]
    args = [pos, gate, dy, x, h1, h3, w1, w3, w2]
    if prev is not None:
        in_specs += [whole(d, f), whole(d, f), whole(f, d)]
        args += list(prev)
    return pl.pallas_call(
        functools.partial(expert_kernel, prev is None),
        grid=(units,),
        in_specs=in_specs,
        out_specs=[pl.BlockSpec((rows, d), lambda i: (i, 0)), whole(d, f), whole(d, f), whole(f, d)],
        out_shape=[jax.ShapeDtypeStruct(x.shape, BF16), jax.ShapeDtypeStruct((d, f), F32), jax.ShapeDtypeStruct((d, f), F32), jax.ShapeDtypeStruct((f, d), F32)],
        compiler_params=pltpu.CompilerParams(dimension_semantics=('arbitrary',), vmem_limit_bytes=56 * 2**20),
        cost_estimate=pl.CostEstimate(flops=15 * 2 * x.shape[0] * d * f, bytes_accessed=60 * 2**20, transcendentals=0),
        name='expert')(*args)


def combine_kernel(idx, rows_ref, out, acc):
    u = pl.program_id(0)
    rows = rows_ref.shape[0]
    tokens = idx.shape[0]
    want = lax.broadcasted_iota(jnp.int32, (tokens, rows), 1) + u * rows
    hit = want == idx[:, 0:1]
    for j in range(1, idx.shape[1]):
        hit = hit | (want == idx[:, j:j + 1])
    part = dot_nn(jnp.where(hit, 1.0, 0.0).astype(BF16), rows_ref[...])

    @pl.when(u == 0)
    def _():
        acc[...] = part

    @pl.when(u > 0)
    def _():
        acc[...] += part

    @pl.when(u == pl.num_programs(0) - 1)
    def _():
        out[...] = acc[...].astype(BF16)


def combine_call(idx, rows, units):
    tokens, d = idx.shape[0], rows.shape[1]
    step = rows.shape[0] // units
    return pl.pallas_call(
        combine_kernel,
        grid=(units,),
        in_specs=[pl.BlockSpec(idx.shape, lambda i: (0, 0)), pl.BlockSpec((step, d), lambda i: (i, 0))],
        out_specs=pl.BlockSpec((tokens, d), lambda i: (0, 0)),
        out_shape=jax.ShapeDtypeStruct((tokens, d), BF16),
        scratch_shapes=[pltpu.VMEM((tokens, d), F32)],
        compiler_params=pltpu.CompilerParams(dimension_semantics=('arbitrary',)),
        cost_estimate=pl.CostEstimate(flops=2 * tokens * rows.shape[0] * d, bytes_accessed=8 * 2**20, transcendentals=0),
        name='combine')(idx, rows)


def solution(mesh):
    group = mesh.shape['ep']
    tok_spec = P(None, ('dp', 'ep'))
    w_spec = P('ep')
    grad_w_spec = P(('dp', 'ep'))

    def local_step(grad_out, expert_out, gate_vals, topk_idx, slot_idx, x_dispatch, h1_pre, h3_pre, w_gate, w_up, w_down):
        n_micro, tokens, top_k, d = expert_out.shape
        experts = group * w_gate.shape[0]
        capacity = x_dispatch.shape[2] // group
        units = group // 2
        me = lax.axis_index('ep')

        all_dy = [lax.all_gather(grad_out[m], 'ep', axis=0).reshape(units, 2 * tokens, d) for m in range(n_micro)]

        idx_t = jnp.swapaxes(topk_idx, 1, 2)[:, :, None, :]
        slot_t = jnp.swapaxes(slot_idx, 1, 2)[:, :, None, :]
        gate_t = jnp.swapaxes(gate_vals, 1, 2)[:, :, None, :]
        match = idx_t == jnp.arange(experts, dtype=jnp.int32)[None, None, :, None]
        slot_map = jnp.max(jnp.where(match, slot_t, -1), axis=1)
        pos_map = jnp.where(slot_map >= 0, slot_map + capacity * lax.rem(me, 2), -1).astype(F32)
        gate_map = jnp.sum(jnp.where(match, gate_t, 0.0), axis=1)
        maps = jnp.stack([pos_map, gate_map], axis=1)
        maps = jnp.moveaxis(maps, 2, 0).reshape(experts, 2 * n_micro, tokens)
        maps = lax.all_to_all(maps, 'ep', 0, 0, tiled=True)
        maps = jnp.moveaxis(maps, 1, 0).reshape(n_micro, 2, units, 1, 2 * tokens)
        send_rows = jnp.where(slot_idx >= 0, topk_idx * capacity + slot_idx, -1)

        grad_gate = jnp.sum(grad_out[:, :, None, :].astype(F32) * expert_out.astype(F32), axis=-1)

        prev = None
        dx = []
        for m in range(n_micro):
            rows, g1, g3, g2 = expert_call(maps[m, 0], maps[m, 1], all_dy[m], x_dispatch[m, 0], h1_pre[m, 0], h3_pre[m, 0], w_gate[0], w_up[0], w_down[0], prev)
            prev = (g1, g3, g2)
            back = lax.all_to_all(rows.reshape(group, capacity, d), 'ep', 0, 0, tiled=True)
            dx.append(combine_call(send_rows[m], back.reshape(experts * capacity, d), units))
        return jnp.stack(dx), grad_gate, prev[0][None], prev[1][None], prev[2][None]

    in_specs = (tok_spec, tok_spec, tok_spec, tok_spec, tok_spec, tok_spec, tok_spec, tok_spec, w_spec, w_spec, w_spec)
    out_specs = (tok_spec, tok_spec, grad_w_spec, grad_w_spec, grad_w_spec)
    return jax.shard_map(local_step, mesh=mesh, in_specs=in_specs, out_specs=out_specs, check_vma=False)
```

```python
import functools
import jax
import jax.numpy as jnp
from jax import lax
from jax.experimental import pallas as pl
from jax.experimental.pallas import tpu as pltpu
from jax.sharding import PartitionSpec as P

F32 = jnp.float32
BF16 = jnp.bfloat16
MESH = pl.DeviceIdType.MESH
SIDE = 4
ORDER = ((0, 0), (1, 0), (3, 0), (0, 1), (0, 3), (1, 1), (3, 3), (1, 3), (3, 1), (2, 0), (0, 2), (2, 1), (1, 2), (2, 3), (3, 2), (2, 2))
UNITS = len(ORDER)


def dot_nn(a, b):
    return lax.dot_general(a, b, (((1,), (0,)), ((), ())), preferred_element_type=F32)


def dot_nt(a, b):
    return lax.dot_general(a, b, (((1,), (1,)), ((), ())), preferred_element_type=F32)


def dot_tn(a, b):
    return lax.dot_general(a, b, (((0,), (0,)), ((), ())), preferred_element_type=F32)


def gather_rows(pos, gate, dy, rows):
    tokens = pos.shape[1]
    hit = lax.broadcasted_iota(jnp.int32, (rows, tokens), 0).astype(F32) == pos
    gate_col = jnp.sum(jnp.where(hit, gate, 0.0), axis=1, keepdims=True)
    onehot = jnp.where(hit, 1.0, 0.0).astype(BF16)
    return (dot_nn(onehot, dy) * gate_col).astype(BF16)


def swiglu_grads(dyd, h1, h3, w2):
    h1 = h1.astype(F32)
    h3 = h3.astype(F32)
    sig = jax.nn.sigmoid(h1)
    silu = h1 * sig
    act = (silu * h3).astype(BF16)
    da = dot_nt(dyd, w2).astype(BF16).astype(F32)
    dh1 = (da * h3 * sig * (1.0 + h1 * (1.0 - sig))).astype(BF16)
    dh3 = (da * silu).astype(BF16)
    return act, dh1, dh3


class Place:
    def __init__(self):
        self.me = lax.axis_index('ep')
        self.core = lax.rem(self.me, 2)
        self.chip = self.me // 2
        self.x = lax.rem(self.chip, SIDE)
        self.y = self.chip // SIDE
        self.partner = self.me + 1 - 2 * self.core

    def chip_at(self, ox, oy):
        return lax.rem(self.y + oy + SIDE, SIDE) * SIDE + lax.rem(self.x + ox + SIDE, SIDE)

    def dev(self, ox, oy):
        return self.chip_at(ox, oy) * 2 + self.core


def pick(k, values):
    out = jnp.int32(values[0])
    for j in range(1, len(values)):
        out = jnp.where(k == j, jnp.int32(values[j]), out)
    return out


class Gather:
    AXES = (((1, 0), (0, 1)), ((0, 1), (1, 0)))

    def __init__(self, place, src, out, ssem, rsem):
        self.p, self.src, self.out, self.ssem, self.rsem = place, src, out, ssem, rsem
        self.half = src.shape[0] // 2
        self.sent = []
        self.ids = {}

    def rows(self, h, q=None):
        if q is None:
            return (h * self.half, self.half)
        return (h * self.half + q * (self.half // 2), self.half // 2)

    def rid(self, *key):
        return self.ids.setdefault(key, len(self.ids))

    def send(self, origin, rows, to, rid, own=False):
        k = len(self.sent)
        cut = pl.ds(*rows)
        self.sent.append(rows[1])
        pltpu.make_async_remote_copy(
            src_ref=self.src.at[cut] if own else self.out.at[origin, cut],
            dst_ref=self.out.at[origin, cut],
            send_sem=self.ssem.at[k], recv_sem=self.rsem.at[rid],
            device_id={'ep': to}, device_id_type=MESH).start()

    def wait(self, rows, rid):
        ref = self.out.at[0, pl.ds(*rows)]
        pltpu.make_async_remote_copy(src_ref=ref, dst_ref=ref, send_sem=self.ssem.at[0], recv_sem=self.rsem.at[rid],
                                     device_id={'ep': self.p.partner}, device_id_type=MESH).wait_recv()

    def to_partner(self, ox, oy, rows, own=False):
        self.send(self.p.dev(ox, oy), rows, self.p.partner, self.rid('p', ox % SIDE, oy % SIDE, rows), own)

    def begin(self):
        for h in (0, 1):
            e1, e2 = self.AXES[h]
            for s in (1, -1):
                self.send(self.p.me, self.rows(h), self.p.dev(s * e1[0], s * e1[1]), self.rid('1', h, s), True)
            for s in (1, -1):
                self.send(self.p.me, self.rows(h), self.p.dev(s * e2[0], s * e2[1]), self.rid('2', h, s, 0), True)
        self.to_partner(0, 0, (0, 2 * self.half), True)

    def first(self, h):
        e1, e2 = self.AXES[h]
        for s in (1, -1):
            ox, oy = -s * e1[0], -s * e1[1]
            self.wait(self.rows(h), self.rid('1', h, s))
            o = self.p.dev(ox, oy)
            part = self.rows(h, 0 if s == 1 else 1)
            self.send(o, part, self.p.dev(s * e1[0], s * e1[1]), self.rid('1f', h, s))
            for t in (1, -1):
                self.send(o, self.rows(h), self.p.dev(t * e2[0], t * e2[1]), self.rid('2', h, t, -s))
            self.to_partner(ox, oy, self.rows(h))

    def second(self, h, j):
        e1, e2 = self.AXES[h]
        for s in (1, -1):
            ox, oy = j * e1[0] - s * e2[0], j * e1[1] - s * e2[1]
            part = self.rows(h, 0 if s == 1 else 1)
            if j == 2:
                for q in (0, 1):
                    self.wait(self.rows(h, q), self.rid('2', h, s, 2, q))
            else:
                self.wait(self.rows(h), self.rid('2', h, s, j))
            self.send(self.p.dev(ox, oy), part, self.p.dev(s * e2[0], s * e2[1]), self.rid('2f', h, s, j))
            self.to_partner(ox, oy, self.rows(h))

    def first_far(self, h):
        e1, e2 = self.AXES[h]
        ox, oy = 2 * e1[0], 2 * e1[1]
        for s in (1, -1):
            q = 0 if s == 1 else 1
            self.wait(self.rows(h, q), self.rid('1f', h, s))
            for t in (1, -1):
                self.send(self.p.dev(ox, oy), self.rows(h, q), self.p.dev(t * e2[0], t * e2[1]), self.rid('2', h, t, 2, q))
        self.to_partner(ox, oy, self.rows(h))

    def second_far(self, j):
        for h in (0, 1):
            e1, e2 = self.AXES[h]
            ox, oy = j * e1[0] + 2 * e2[0], j * e1[1] + 2 * e2[1]
            for s in (1, -1):
                self.wait(self.rows(h, 0 if s == 1 else 1), self.rid('2f', h, s, j))
            self.to_partner(ox, oy, self.rows(h))

    def from_partner(self, ox, oy):
        parts = [(key[3], r) for key, r in self.ids.items() if key[:3] == ('p', ox, oy)]
        assert sum(rows[1] for rows, _ in parts) == 2 * self.half
        for rows, r in parts:
            self.wait(rows, r)

    def finish(self):
        for k, size in enumerate(self.sent):
            ref = self.out.at[0, pl.ds(0, size)]
            pltpu.make_async_remote_copy(src_ref=ref, dst_ref=ref, send_sem=self.ssem.at[k], recv_sem=self.rsem.at[0],
                                         device_id={'ep': self.p.partner}, device_id_type=MESH).wait_send()


def layer_kernel(group, dy, maps, idx, yd, x, h1, h3, w1, w3, w2,
                 dx_out, dg_out, g1_out, g3_out, g2_out, everyone, staged, back,
                 maps_all, w1_v, w3_v, w2_v, dy_t, h1_t, h3_t, dx_t, yd_t, dyo, x_t, back_t, dyd_s, act_s, dh1_s, dh3_s,
                 g1, g3, g2, acc, idx_b,
                 ag_ssem, ag_rsem, m_ssem, m_rsem, r_ssem, r_rsem, own_sem, w_sem, in_sem, st_sem, yd_sem, x_sem, b_sem, g_sem):
    p = Place()
    me = p.me
    n_micro, tokens, d = dy.shape
    capacity = back.shape[2] // 2
    rows = 2 * capacity
    per_micro = rows * UNITS

    barrier = pltpu.get_barrier_semaphore()

    def greet(k, c):
        pl.semaphore_signal(barrier, inc=1, device_id={'ep': lax.rem(me + k, group)}, device_id_type=MESH)
        return c

    lax.fori_loop(1, group, greet, 0)

    weights = [pltpu.make_async_copy(a, b, w_sem.at[k]) for k, (a, b) in enumerate(((w1, w1_v), (w3, w3_v), (w2, w2_v)))]
    own = [pltpu.make_async_copy(dy.at[m], everyone.at[m, me], own_sem.at[m]) for m in range(n_micro)]
    own_maps = pltpu.make_async_copy(maps.at[me], maps_all.at[me], own_sem.at[n_micro])
    own_dy = pltpu.make_async_copy(dy, dyo, own_sem.at[n_micro + 1])
    own_dy.start()

    yd_tokens = yd_t.shape[1]
    yd_steps = yd.shape[0] // yd_tokens

    def yd_copy(i):
        slot = lax.rem(i, 2)
        return pltpu.make_async_copy(yd.at[pl.ds(i * yd_tokens, yd_tokens)], yd_t.at[slot], yd_sem.at[slot])

    yd_copy(0).start()
    pl.semaphore_wait(barrier, group - 1)

    gathers = [Gather(p, dy.at[m], everyone.at[m], ag_ssem.at[m], ag_rsem.at[m]) for m in range(n_micro)]
    gathers[0].begin()

    def map_copy(to, origin, slot_s, slot_r):
        return pltpu.make_async_remote_copy(src_ref=maps.at[to], dst_ref=maps_all.at[origin], send_sem=m_ssem.at[slot_s],
                                            recv_sem=m_rsem.at[slot_r], device_id={'ep': to}, device_id_type=MESH)

    def send_map(k, c):
        to = lax.rem(me + k, group)
        map_copy(to, me, k, me).start()
        return c

    lax.fori_loop(1, group, send_map, 0)
    own_maps.start()
    for c in own + weights:
        c.start()

    own_dy.wait()

    def gate_step(i, c):
        @pl.when(i + 1 < yd_steps)
        def _():
            yd_copy(i + 1).start()
        yd_copy(i).wait()
        slot = lax.rem(i, 2)
        per = tokens // yd_tokens
        m = i // per
        r0 = pl.multiple_of(lax.rem(i, per) * yd_tokens, yd_tokens)
        a = dyo[m, pl.ds(r0, yd_tokens), :].astype(F32)
        b = yd_t[slot].astype(F32)
        dg_out[pl.ds(pl.multiple_of(i * yd_tokens, yd_tokens), yd_tokens), :] = jnp.sum(a[:, None, :] * b, axis=-1)
        return c

    lax.fori_loop(0, yd_steps, gate_step, 0)

    def spread(m):
        for j in range(idx.shape[2]):
            idx_b[m, j] = jnp.broadcast_to(idx[m, :, j:j + 1], idx_b.shape[2:])

    for m in range(n_micro):
        spread(m)

    def unit_of(i):
        m = i // UNITS
        k = lax.rem(i, UNITS)
        u = p.chip_at(pick(k, [o[0] for o in ORDER]), pick(k, [o[1] for o in ORDER]))
        return m, k, u

    def loads(i):
        m, k, u = unit_of(i)
        slot = lax.rem(i, 2)
        r0 = pl.multiple_of(u * rows, 16)
        return [pltpu.make_async_copy(everyone.at[m, pl.ds(2 * u, 2)], dy_t.at[slot], in_sem.at[slot, 0]),
                pltpu.make_async_copy(h1.at[m, pl.ds(r0, rows)], h1_t.at[slot], in_sem.at[slot, 1]),
                pltpu.make_async_copy(h3.at[m, pl.ds(r0, rows)], h3_t.at[slot], in_sem.at[slot, 2])]

    def stage_copy(i):
        m, k, u = unit_of(i)
        slot = lax.rem(i, 2)
        return pltpu.make_async_copy(dx_t.at[slot], staged.at[m, u], st_sem.at[slot])

    def return_copy(i, w, to, u, m):
        cut = pl.ds(pl.multiple_of(w * capacity, 8), capacity)
        mine = pl.ds(pl.multiple_of(p.core * capacity, 8), capacity)
        return pltpu.make_async_remote_copy(src_ref=staged.at[m, u, cut], dst_ref=back.at[m, p.chip, mine],
                                            send_sem=r_ssem.at[i * 2 + w], recv_sem=r_rsem.at[m * group + me],
                                            device_id={'ep': to}, device_id_type=MESH)

    def own_return(m):
        mine = pl.ds(pl.multiple_of(p.core * capacity, 8), capacity)
        return pltpu.make_async_copy(staged.at[m, p.chip, mine], back.at[m, p.chip, mine], own_sem.at[n_micro + 2 + m])

    def send_back(i):
        m, k, u = unit_of(i)

        @pl.when(k == 0)
        def _():
            return_copy(i, 1 - p.core, p.partner, u, m).start()
            own_return(m).start()

        @pl.when(k > 0)
        def _():
            for w in (0, 1):
                return_copy(i, w, 2 * u + w, u, m).start()

    a, b = gathers
    events = {i: [] for i in range(-1, n_micro * UNITS)}
    events[-1] += [lambda: a.first(0), lambda: a.first(1), lambda: a.second(0, 0), lambda: a.second(1, 0), b.begin]
    events[0] += [lambda: a.first_far(0), lambda: a.first_far(1)]
    events[1] += [lambda: a.second(0, 1), lambda: a.second(1, 1)]
    events[2] += [lambda: a.second(0, -1), lambda: a.second(1, -1)]
    events[4] += [lambda: a.second(0, 2), lambda: a.second(1, 2)]
    events[5] += [lambda: b.first(0), lambda: b.first(1)]
    events[6] += [lambda: b.second(0, 0), lambda: b.second(1, 0)]
    events[8] += [lambda: a.second_far(0)]
    events[9] += [lambda: b.first_far(0), lambda: b.first_far(1)]
    events[10] += [lambda: a.second_far(1), lambda: a.second_far(-1), lambda: a.second_far(2)]
    events[11] += [lambda: b.second(0, 1), lambda: b.second(1, 1)]
    events[12] += [lambda: b.second(0, -1), lambda: b.second(1, -1)]
    events[14] += [lambda: b.second(0, 2), lambda: b.second(1, 2)]
    events[UNITS + 8] += [lambda: b.second_far(0)]
    events[UNITS + 10] += [lambda: b.second_far(1), lambda: b.second_far(-1), lambda: b.second_far(2)]
    for m, g in enumerate(gathers):
        for k, (ox, oy) in enumerate(ORDER):
            events[m * UNITS + k - 1].append(functools.partial(g.from_partner, ox, oy))
        events[m * UNITS - 1].append(own[m].wait)

    for e in events[-1]:
        e()

    def recv_map(k, c):
        s = lax.rem(me + k, group)
        map_copy(s, s, k, s).wait()
        return c

    lax.fori_loop(1, group, recv_map, 0)
    own_maps.wait()
    for c in loads(0):
        c.start()
    for c in weights:
        c.wait()

    total = n_micro * UNITS

    def unit_step(i, c):
        for k in range(total):
            if events[k]:
                @pl.when(i == k)
                def _():
                    for e in events[k]:
                        e()

        @pl.when(i + 1 < total)
        def _():
            for t in loads(i + 1):
                t.start()

        @pl.when(i >= 1)
        def _():
            stage_copy(i - 1).wait()
            send_back(i - 1)

        for t in loads(i):
            t.wait()
        m, k, u = unit_of(i)
        slot = lax.rem(i, 2)
        pos = jnp.concatenate([maps_all[2 * u, 2 * m], maps_all[2 * u + 1, 2 * m]], axis=1)
        gate = jnp.concatenate([maps_all[2 * u, 2 * m + 1], maps_all[2 * u + 1, 2 * m + 1]], axis=1)
        dyd = gather_rows(pos, gate, dy_t[slot].reshape(2 * tokens, d), rows)
        act, dh1, dh3 = swiglu_grads(dyd, h1_t[slot], h3_t[slot], w2_v[...])
        dx_t[slot] = (dot_nt(dh1, w1_v[...]) + dot_nt(dh3, w3_v[...])).astype(BF16)
        stage_copy(i).start()
        at = pl.ds(pl.multiple_of(m * per_micro + u * rows, 16), rows)
        dyd_s[at, :] = dyd
        act_s[at, :] = act
        dh1_s[at, :] = dh1
        dh3_s[at, :] = dh3
        return c

    lax.fori_loop(0, total, unit_step, 0)
    stage_copy(total - 1).wait()
    send_back(total - 1)

    depth = x_t.shape[1]
    x_steps = n_micro * per_micro // depth

    def x_copy(i):
        slot = lax.rem(i, 2)
        return pltpu.make_async_copy(x.at[pl.ds(pl.multiple_of(i * depth, depth), depth)], x_t.at[slot], x_sem.at[slot])

    x_copy(0).start()
    for g in (g1, g3, g2):
        g[...] = jnp.zeros_like(g)

    def weight_step(i, c):
        @pl.when(i + 1 < x_steps)
        def _():
            x_copy(i + 1).start()
        x_copy(i).wait()
        at = pl.ds(pl.multiple_of(i * depth, depth), depth)
        xt = x_t[lax.rem(i, 2)]
        g1[...] += dot_tn(xt, dh1_s[at, :])
        g3[...] += dot_tn(xt, dh3_s[at, :])
        g2[...] += dot_tn(act_s[at, :], dyd_s[at, :])
        return c

    lax.fori_loop(0, x_steps, weight_step, 0)
    outs = [pltpu.make_async_copy(s, t, g_sem.at[k]) for k, (s, t) in enumerate(((g1, g1_out), (g3, g3_out), (g2, g2_out)))]
    for c in outs:
        c.start()

    def arrive(i):
        m, k, u = unit_of(i)

        def wait_from(s):
            cut = pl.ds(0, capacity)
            pltpu.make_async_remote_copy(src_ref=back.at[m, u, cut], dst_ref=back.at[m, u, cut], send_sem=r_ssem.at[0],
                                         recv_sem=r_rsem.at[m * group + s], device_id={'ep': p.partner}, device_id_type=MESH).wait_recv()

        @pl.when(k == 0)
        def _():
            wait_from(p.partner)
            own_return(m).wait()

        @pl.when(k > 0)
        def _():
            wait_from(2 * u)
            wait_from(2 * u + 1)

    def back_copy(i):
        m, k, u = unit_of(i)
        slot = lax.rem(i, 2)
        return pltpu.make_async_copy(back.at[m, u], back_t.at[slot], b_sem.at[slot])

    arrive(0)
    back_copy(0).start()

    def combine_step(i, c):
        @pl.when(i + 1 < total)
        def _():
            arrive(i + 1)
            back_copy(i + 1).start()
        back_copy(i).wait()
        m, k, u = unit_of(i)
        lanes = idx_b.shape[3]
        base = u * rows
        hits = []
        for c0 in range(0, rows, lanes):
            want = lax.broadcasted_iota(jnp.int32, (tokens, lanes), 1) + (base + c0)
            hit = idx_b[m, 0] == want
            for j in range(1, idx_b.shape[1]):
                hit = hit | (idx_b[m, j] == want)
            hits.append(jnp.where(hit, 1.0, 0.0))
        sel = jnp.concatenate(hits, axis=1)[:, :rows].astype(BF16)
        part = dot_nn(sel, back_t[lax.rem(i, 2)])

        @pl.when(k == 0)
        def _():
            acc[...] = part

        @pl.when(k > 0)
        def _():
            acc[...] += part

        @pl.when(k == UNITS - 1)
        def _():
            dx_out[m] = acc[...].astype(BF16)
        return c

    lax.fori_loop(0, total, combine_step, 0)

    for g in gathers:
        g.finish()

    def sent(i, c):
        m, k, u = unit_of(i)

        @pl.when(k == 0)
        def _():
            return_copy(i, 1 - p.core, p.partner, u, m).wait_send()

        @pl.when(k > 0)
        def _():
            for w in (0, 1):
                return_copy(i, w, 2 * u + w, u, m).wait_send()
        return c

    lax.fori_loop(0, total, sent, 0)
    for c in outs:
        c.wait()


def layer_call(group, dy, maps, idx, yd, x, h1, h3, w1, w3, w2):
    n_micro, tokens, d = dy.shape
    f = h1.shape[2]
    rows = h1.shape[1] // UNITS
    saved = n_micro * h1.shape[1]
    hbm = pl.BlockSpec(memory_space=pltpu.HBM)
    vmem = pl.BlockSpec(memory_space=pltpu.VMEM)
    dma = pltpu.SemaphoreType.DMA
    out = pl.pallas_call(
        functools.partial(layer_kernel, group),
        in_specs=[hbm, hbm, vmem, hbm, hbm, hbm, hbm, hbm, hbm, hbm],
        out_specs=[vmem, vmem, hbm, hbm, hbm, hbm, hbm, hbm],
        out_shape=[jax.ShapeDtypeStruct((n_micro, tokens, d), BF16),
                   jax.ShapeDtypeStruct((n_micro * tokens, yd.shape[1]), F32),
                   jax.ShapeDtypeStruct((d, f), F32), jax.ShapeDtypeStruct((d, f), F32), jax.ShapeDtypeStruct((f, d), F32),
                   jax.ShapeDtypeStruct((n_micro, group, tokens, d), BF16),
                   jax.ShapeDtypeStruct((n_micro, UNITS, rows, d), BF16),
                   jax.ShapeDtypeStruct((n_micro, UNITS, rows, d), BF16)],
        scratch_shapes=[pltpu.VMEM(maps.shape, F32),
                        pltpu.VMEM((d, f), BF16), pltpu.VMEM((d, f), BF16), pltpu.VMEM((f, d), BF16),
                        pltpu.VMEM((2, 2, tokens, d), BF16), pltpu.VMEM((2, rows, f), BF16), pltpu.VMEM((2, rows, f), BF16),
                        pltpu.VMEM((2, rows, d), BF16), pltpu.VMEM((2, 32) + yd.shape[1:], BF16), pltpu.VMEM(dy.shape, BF16),
                        pltpu.VMEM((2, 256, d), BF16), pltpu.VMEM((2, rows, d), BF16),
                        pltpu.VMEM((saved, d), BF16), pltpu.VMEM((saved, f), BF16), pltpu.VMEM((saved, f), BF16), pltpu.VMEM((saved, f), BF16),
                        pltpu.VMEM((d, f), F32), pltpu.VMEM((d, f), F32), pltpu.VMEM((f, d), F32),
                        pltpu.VMEM((tokens, d), F32), pltpu.VMEM((n_micro, idx.shape[2], tokens, 128), jnp.int32),
                        dma((n_micro, 80)), dma((n_micro, 80)), dma((group,)), dma((group,)),
                        dma((2 * n_micro * UNITS,)), dma((n_micro * group,)), dma((n_micro + 2 + n_micro,)), dma((3,)),
                        dma((2, 3)), dma((2,)), dma((2,)), dma((2,)), dma((2,)), dma((3,))],
        compiler_params=pltpu.CompilerParams(collective_id=0, has_side_effects=True, vmem_limit_bytes=64 * 2**20 - 2**17),
        name='layer')(dy, maps, idx, yd, x, h1, h3, w1, w3, w2)
    return out[:5]


def solution(mesh):
    group = mesh.shape['ep']
    tok_spec = P(None, ('dp', 'ep'))
    w_spec = P('ep')
    grad_w_spec = P(('dp', 'ep'))

    def local_step(grad_out, expert_out, gate_vals, topk_idx, slot_idx, x_dispatch, h1_pre, h3_pre, w_gate, w_up, w_down):
        n_micro, tokens, top_k, d = expert_out.shape
        experts = group * w_gate.shape[0]
        capacity = x_dispatch.shape[2] // group
        me = lax.axis_index('ep')
        idx_t = jnp.swapaxes(topk_idx, 1, 2)[:, :, None, :]
        slot_t = jnp.swapaxes(slot_idx, 1, 2)[:, :, None, :]
        gate_t = jnp.swapaxes(gate_vals, 1, 2)[:, :, None, :]
        match = idx_t == jnp.arange(experts, dtype=jnp.int32)[None, None, :, None]
        slot_map = jnp.max(jnp.where(match, slot_t, -1), axis=1)
        pos_map = jnp.where(slot_map >= 0, slot_map + capacity * lax.rem(me, 2), -1).astype(F32)
        gate_map = jnp.sum(jnp.where(match, gate_t, 0.0), axis=1)
        maps = jnp.stack([pos_map, gate_map], axis=1)
        maps = jnp.moveaxis(maps, 2, 0).reshape(experts, 2 * n_micro, 1, tokens)
        send_rows = jnp.where(slot_idx >= 0, topk_idx * capacity + slot_idx, -1)
        dx, dg, g1, g3, g2 = layer_call(
            group, grad_out, maps, send_rows, expert_out.reshape(n_micro * tokens, top_k, d),
            x_dispatch.reshape(-1, d), h1_pre[:, 0], h3_pre[:, 0], w_gate[0], w_up[0], w_down[0])
        return dx, dg.reshape(n_micro, tokens, top_k), g1[None], g3[None], g2[None]

    in_specs = (tok_spec, tok_spec, tok_spec, tok_spec, tok_spec, tok_spec, tok_spec, tok_spec, w_spec, w_spec, w_spec)
    out_specs = (tok_spec, tok_spec, grad_w_spec, grad_w_spec, grad_w_spec)
    return jax.shard_map(local_step, mesh=mesh, in_specs=in_specs, out_specs=out_specs, check_vma=False)
```

```python
import functools
import jax
import jax.numpy as jnp
from jax import lax
from jax.experimental import pallas as pl
from jax.experimental.pallas import tpu as pltpu
from jax.sharding import PartitionSpec as P

F32 = jnp.float32
BF16 = jnp.bfloat16
MESH = pl.DeviceIdType.MESH
SIDE = 4
ORDER = ((0, 0), (1, 0), (3, 0), (0, 1), (0, 3), (1, 1), (3, 3), (1, 3), (3, 1), (2, 0), (0, 2), (2, 1), (1, 2), (2, 3), (3, 2), (2, 2))
UNITS = len(ORDER)
FAR_FIRST = ((0, 2), (1, 2), (3, 2), (2, 2), (2, 0), (2, 1), (2, 3), (0, 1), (1, 1), (3, 1), (1, 0), (1, 3), (0, 3), (3, 3), (3, 0), (0, 0))
PART_ORDER = (2, 1, 3, 0)


def dot_nn(a, b):
    return lax.dot_general(a, b, (((1,), (0,)), ((), ())), preferred_element_type=F32)


def dot_nt(a, b):
    return lax.dot_general(a, b, (((1,), (1,)), ((), ())), preferred_element_type=F32)


def dot_tn(a, b):
    return lax.dot_general(a, b, (((0,), (0,)), ((), ())), preferred_element_type=F32)


def gather_rows(pos, gate, dy, rows):
    tokens = pos.shape[1]
    hit = lax.broadcasted_iota(jnp.int32, (rows, tokens), 0).astype(F32) == pos
    gate_col = jnp.sum(jnp.where(hit, gate, 0.0), axis=1, keepdims=True)
    onehot = jnp.where(hit, 1.0, 0.0).astype(BF16)
    return (dot_nn(onehot, dy) * gate_col).astype(BF16)


def swiglu_grads(dyd, h1, h3, w2):
    h1 = h1.astype(F32)
    h3 = h3.astype(F32)
    sig = jax.nn.sigmoid(h1)
    silu = h1 * sig
    act = (silu * h3).astype(BF16)
    da = dot_nt(dyd, w2).astype(BF16).astype(F32)
    dh1 = (da * h3 * sig * (1.0 + h1 * (1.0 - sig))).astype(BF16)
    dh3 = (da * silu).astype(BF16)
    return act, dh1, dh3


class Place:
    def __init__(self):
        self.me = lax.axis_index('ep')
        self.core = lax.rem(self.me, 2)
        self.chip = self.me // 2
        self.x = lax.rem(self.chip, SIDE)
        self.y = self.chip // SIDE
        self.partner = self.me + 1 - 2 * self.core

    def chip_at(self, ox, oy):
        return lax.rem(self.y + oy + SIDE, SIDE) * SIDE + lax.rem(self.x + ox + SIDE, SIDE)

    def dev(self, ox, oy):
        return self.chip_at(ox, oy) * 2 + self.core


def pick(k, values):
    out = jnp.int32(values[0])
    for j in range(1, len(values)):
        out = jnp.where(k == j, jnp.int32(values[j]), out)
    return out


class Gather:
    AXES = (((1, 0), (0, 1)), ((0, 1), (1, 0)))

    def __init__(self, place, src, out, ssem, rsem):
        self.p, self.src, self.out, self.ssem, self.rsem = place, src, out, ssem, rsem
        self.half = src.shape[0] // 2
        self.sent = []
        self.ids = {}

    def rows(self, h, q=None):
        if q is None:
            return (h * self.half, self.half)
        return (h * self.half + q * (self.half // 2), self.half // 2)

    def rid(self, *key):
        return self.ids.setdefault(key, len(self.ids))

    def send(self, origin, rows, to, rid, own=False):
        k = len(self.sent)
        cut = pl.ds(*rows)
        self.sent.append(rows[1])
        pltpu.make_async_remote_copy(
            src_ref=self.src.at[cut] if own else self.out.at[origin, cut],
            dst_ref=self.out.at[origin, cut],
            send_sem=self.ssem.at[k], recv_sem=self.rsem.at[rid],
            device_id={'ep': to}, device_id_type=MESH).start()

    def wait(self, rows, rid):
        ref = self.out.at[0, pl.ds(*rows)]
        pltpu.make_async_remote_copy(src_ref=ref, dst_ref=ref, send_sem=self.ssem.at[0], recv_sem=self.rsem.at[rid],
                                     device_id={'ep': self.p.partner}, device_id_type=MESH).wait_recv()

    def to_partner(self, ox, oy, rows, own=False):
        self.send(self.p.dev(ox, oy), rows, self.p.partner, self.rid('p', ox % SIDE, oy % SIDE, rows), own)

    def begin(self):
        for h in (0, 1):
            e1, e2 = self.AXES[h]
            for s in (1, -1):
                self.send(self.p.me, self.rows(h), self.p.dev(s * e1[0], s * e1[1]), self.rid('1', h, s), True)
            for s in (1, -1):
                self.send(self.p.me, self.rows(h), self.p.dev(s * e2[0], s * e2[1]), self.rid('2', h, s, 0), True)
        self.to_partner(0, 0, (0, 2 * self.half), True)

    def first(self, h):
        e1, e2 = self.AXES[h]
        for s in (1, -1):
            ox, oy = -s * e1[0], -s * e1[1]
            self.wait(self.rows(h), self.rid('1', h, s))
            o = self.p.dev(ox, oy)
            part = self.rows(h, 0 if s == 1 else 1)
            self.send(o, part, self.p.dev(s * e1[0], s * e1[1]), self.rid('1f', h, s))
            for t in (1, -1):
                self.send(o, self.rows(h), self.p.dev(t * e2[0], t * e2[1]), self.rid('2', h, t, -s))
            self.to_partner(ox, oy, self.rows(h))

    def second(self, h, j):
        e1, e2 = self.AXES[h]
        for s in (1, -1):
            ox, oy = j * e1[0] - s * e2[0], j * e1[1] - s * e2[1]
            part = self.rows(h, 0 if s == 1 else 1)
            if j == 2:
                for q in (0, 1):
                    self.wait(self.rows(h, q), self.rid('2', h, s, 2, q))
            else:
                self.wait(self.rows(h), self.rid('2', h, s, j))
            self.send(self.p.dev(ox, oy), part, self.p.dev(s * e2[0], s * e2[1]), self.rid('2f', h, s, j))
            self.to_partner(ox, oy, self.rows(h))

    def first_far(self, h):
        e1, e2 = self.AXES[h]
        ox, oy = 2 * e1[0], 2 * e1[1]
        for s in (1, -1):
            q = 0 if s == 1 else 1
            self.wait(self.rows(h, q), self.rid('1f', h, s))
            for t in (1, -1):
                self.send(self.p.dev(ox, oy), self.rows(h, q), self.p.dev(t * e2[0], t * e2[1]), self.rid('2', h, t, 2, q))
        self.to_partner(ox, oy, self.rows(h))

    def second_far(self, j):
        for h in (0, 1):
            e1, e2 = self.AXES[h]
            ox, oy = j * e1[0] + 2 * e2[0], j * e1[1] + 2 * e2[1]
            for s in (1, -1):
                self.wait(self.rows(h, 0 if s == 1 else 1), self.rid('2f', h, s, j))
            self.to_partner(ox, oy, self.rows(h))

    def from_partner(self, ox, oy):
        parts = [(key[3], r) for key, r in self.ids.items() if key[:3] == ('p', ox, oy)]
        assert sum(rows[1] for rows, _ in parts) == 2 * self.half
        for rows, r in parts:
            self.wait(rows, r)

    def finish(self):
        for k, size in enumerate(self.sent):
            ref = self.out.at[0, pl.ds(0, size)]
            pltpu.make_async_remote_copy(src_ref=ref, dst_ref=ref, send_sem=self.ssem.at[k], recv_sem=self.rsem.at[0],
                                         device_id={'ep': self.p.partner}, device_id_type=MESH).wait_send()


def layer_kernel(group, dy, topk, slots, gates, yd, x, h1, h3, w1, w3, w2,
                 dx_out, dg_out, g1_out, g3_out, g2_out, everyone, staged, lined, parts,
                 maps, maps_all, idx_all, w1_v, w3_v, w2_v, dy_t, h1_t, h3_t, dx_t, yd_t, dyo, x_t, line_t, sum_s, part_t,
                 dyd_s, act_s, dh1_s, dh3_s, g1, g3, g2,
                 ag_ssem, ag_rsem, m_ssem, m_rsem, i_ssem, i_rsem, r_ssem, r_rsem, p_ssem, p_rsem,
                 own_sem, w_sem, in_sem, st_sem, yd_sem, x_sem, l_sem, f_sem, g_sem):
    p = Place()
    me = p.me
    n_micro, tokens, d = dy.shape
    top_k = topk.shape[1]
    rows = lined.shape[4]
    capacity = rows // 2
    wide = d // 2
    per_micro = rows * UNITS

    barrier = pltpu.get_barrier_semaphore()

    def greet(k, c):
        pl.semaphore_signal(barrier, inc=1, device_id={'ep': lax.rem(me + k, group)}, device_id_type=MESH)
        return c

    lax.fori_loop(1, group, greet, 0)

    weights = [pltpu.make_async_copy(a, b, w_sem.at[k]) for k, (a, b) in enumerate(((w1, w1_v), (w3, w3_v), (w2, w2_v)))]
    own = [pltpu.make_async_copy(dy.at[m], everyone.at[m, me], own_sem.at[m]) for m in range(n_micro)]
    own_dy = pltpu.make_async_copy(dy, dyo, own_sem.at[n_micro])
    own_dy.start()
    yd_tokens = yd_t.shape[1]
    yd_steps = yd.shape[0] // yd_tokens

    def yd_copy(i):
        slot = lax.rem(i, 2)
        return pltpu.make_async_copy(yd.at[pl.ds(i * yd_tokens, yd_tokens)], yd_t.at[slot], yd_sem.at[slot])

    yd_copy(0).start()

    for m in range(n_micro):
        experts = lax.broadcasted_iota(jnp.int32, (group, tokens), 0)
        pos = jnp.full((group, tokens), -1, jnp.int32)
        gate = jnp.zeros((group, tokens), F32)
        for j in range(top_k):
            same = experts == topk[m, j:j + 1, :]
            at = slots[m, j:j + 1, :]
            pos = jnp.where(same, jnp.where(at >= 0, at + p.core * capacity, -1), pos)
            gate = jnp.where(same, gates[m, j:j + 1, :], gate)
        pos = pos.astype(F32)
        for e in range(group):
            maps[e, 2 * m] = pos[e:e + 1, :]
            maps[e, 2 * m + 1] = gate[e:e + 1, :]
        mine = jnp.where(slots[m] >= 0, topk[m] * capacity + slots[m], -1)
        idx_all[p.y, m] = mine
        idx_all[SIDE + p.x, m] = mine
    maps_all[me] = maps[me]

    pl.semaphore_wait(barrier, group - 1)

    gathers = [Gather(p, dy.at[m], everyone.at[m], ag_ssem.at[m], ag_rsem.at[m]) for m in range(n_micro)]
    gathers[0].begin()

    def map_copy(to, origin, slot_s, slot_r):
        return pltpu.make_async_remote_copy(src_ref=maps.at[to], dst_ref=maps_all.at[origin], send_sem=m_ssem.at[slot_s],
                                            recv_sem=m_rsem.at[slot_r], device_id={'ep': to}, device_id_type=MESH)

    def send_map(k, c):
        to = lax.rem(me + k, group)
        map_copy(to, me, k, me).start()
        return c

    lax.fori_loop(1, group, send_map, 0)

    def idx_copy(half, o):
        at = p.y if half == 0 else SIDE + p.x
        to = p.dev(0, o) if half == 0 else p.dev(o, 0)
        return pltpu.make_async_remote_copy(src_ref=idx_all.at[at], dst_ref=idx_all.at[at], send_sem=i_ssem.at[half * SIDE + o],
                                            recv_sem=i_rsem.at[at], device_id={'ep': to}, device_id_type=MESH)

    def idx_wait(half, o):
        at = lax.rem(p.y + o, SIDE) if half == 0 else SIDE + lax.rem(p.x + o, SIDE)
        pltpu.make_async_remote_copy(src_ref=idx_all.at[at], dst_ref=idx_all.at[at], send_sem=i_ssem.at[0], recv_sem=i_rsem.at[at],
                                     device_id={'ep': p.partner}, device_id_type=MESH).wait_recv()

    for half in (0, 1):
        for o in range(1, SIDE):
            idx_copy(half, o).start()
    for c in own + weights:
        c.start()

    own_dy.wait()

    def gate_step(i, c):
        @pl.when(i + 1 < yd_steps)
        def _():
            yd_copy(i + 1).start()
        yd_copy(i).wait()
        slot = lax.rem(i, 2)
        per = tokens // yd_tokens
        m = i // per
        at = pl.ds(pl.multiple_of(lax.rem(i, per) * yd_tokens, yd_tokens), yd_tokens)
        fine = 32
        out = []
        for r0 in range(0, yd_tokens, fine):
            a = dyo[m, pl.ds(pl.multiple_of(lax.rem(i, per) * yd_tokens + r0, fine), fine), :].astype(F32)
            b = yd_t[slot, r0:r0 + fine].astype(F32)
            out.append(jnp.sum(a[:, None, :] * b, axis=-1))
        dg_out[m, :, at] = jnp.concatenate(out, axis=0).T
        return c

    lax.fori_loop(0, yd_steps, gate_step, 0)

    def chip_of(order, i):
        ox, oy = pick(i, [o[0] for o in order]), pick(i, [o[1] for o in order])
        return lax.rem(p.x + ox, SIDE), lax.rem(p.y + oy, SIDE)

    class Units:
        def __init__(self, m, order):
            self.m, self.order = m, order

        def loads(self, i):
            cx, cy = chip_of(self.order, i)
            u = cy * SIDE + cx
            slot = lax.rem(i, 2)
            cut = pl.ds(pl.multiple_of(u * rows, 16), rows)
            return [pltpu.make_async_copy(everyone.at[self.m, pl.ds(2 * u, 2)], dy_t.at[slot], in_sem.at[slot, 0]),
                    pltpu.make_async_copy(h1.at[self.m, cut], h1_t.at[slot], in_sem.at[slot, 1]),
                    pltpu.make_async_copy(h3.at[self.m, cut], h3_t.at[slot], in_sem.at[slot, 2])]

        def stage(self, i):
            cx, cy = chip_of(self.order, i)
            slot = lax.rem(i, 2)
            return pltpu.make_async_copy(dx_t.at[slot], staged.at[self.m, cy * SIDE + cx], st_sem.at[slot])

        def refs(self, i, half, w):
            cx, cy = chip_of(self.order, i)
            src = staged.at[self.m, cy * SIDE + cx, pl.ds(pl.multiple_of(w * capacity, 8), capacity), pl.ds(half * wide, wide)]
            mine = pl.ds(pl.multiple_of(p.core * capacity, 8), capacity)
            place = cy if half == 0 else cx
            came = p.x if half == 0 else p.y
            dst = lined.at[self.m, half, place, came, mine]
            sem = r_rsem.at[self.m, half, place, came * 2 + p.core]
            chip = p.y * SIDE + cx if half == 0 else cy * SIDE + p.x
            here = (cx == p.x) if half == 0 else (cy == p.y)
            return src, dst, sem, chip * 2 + w, here

        def each(self, i, act):
            for half in (0, 1):
                for w in (0, 1):
                    src, dst, sem, to, here = self.refs(i, half, w)
                    remote = pltpu.make_async_remote_copy(src_ref=src, dst_ref=dst, send_sem=r_ssem.at[self.m, i * 4 + half * 2 + w], recv_sem=sem,
                                                          device_id={'ep': to}, device_id_type=MESH)
                    self_too = jnp.logical_and(here, p.core == w)

                    @pl.when(jnp.logical_not(self_too))
                    def _():
                        act(remote)

                    if act is START:
                        @pl.when(self_too)
                        def _():
                            pltpu.make_async_copy(src, dst, sem).start()

        def run(self, events):
            for t in self.loads(0):
                t.start()

            def step(i, c):
                for k in range(UNITS):
                    if events.get(k):
                        @pl.when(i == k)
                        def _():
                            for e in events[k]:
                                e()

                @pl.when(i + 1 < UNITS)
                def _():
                    for t in self.loads(i + 1):
                        t.start()

                @pl.when(i >= 1)
                def _():
                    self.stage(i - 1).wait()
                    self.each(i - 1, START)

                for t in self.loads(i):
                    t.wait()
                m = self.m
                cx, cy = chip_of(self.order, i)
                u = cy * SIDE + cx
                slot = lax.rem(i, 2)
                pos = jnp.concatenate([maps_all[2 * u, 2 * m], maps_all[2 * u + 1, 2 * m]], axis=1)
                gate = jnp.concatenate([maps_all[2 * u, 2 * m + 1], maps_all[2 * u + 1, 2 * m + 1]], axis=1)
                dyd = gather_rows(pos, gate, dy_t[slot].reshape(2 * tokens, d), rows)
                act, dh1, dh3 = swiglu_grads(dyd, h1_t[slot], h3_t[slot], w2_v[...])
                dx_t[slot] = (dot_nt(dh1, w1_v[...]) + dot_nt(dh3, w3_v[...])).astype(BF16)
                self.stage(i).start()
                at = pl.ds(pl.multiple_of(u * rows, 16), rows)
                dyd_s[at, :] = dyd
                act_s[at, :] = act
                dh1_s[at, :] = dh1
                dh3_s[at, :] = dh3
                return c

            lax.fori_loop(0, UNITS, step, 0)
            self.stage(UNITS - 1).wait()
            self.each(UNITS - 1, START)

        def finish(self):
            def step(i, c):
                self.each(i, WAIT_SEND)
                return c
            lax.fori_loop(0, UNITS, step, 0)

    depth = x_t.shape[1]
    x_steps = per_micro // depth

    def weight_grads(m, events):
        def x_copy(i):
            slot = lax.rem(i, 2)
            return pltpu.make_async_copy(x.at[m, pl.ds(pl.multiple_of(i * depth, depth), depth)], x_t.at[slot], x_sem.at[slot])

        x_copy(0).start()

        def step(i, c):
            for k in range(x_steps):
                if events.get(k):
                    @pl.when(i == k)
                    def _():
                        for e in events[k]:
                            e()

            @pl.when(i + 1 < x_steps)
            def _():
                x_copy(i + 1).start()
            x_copy(i).wait()
            at = pl.ds(pl.multiple_of(i * depth, depth), depth)
            xt = x_t[lax.rem(i, 2)]
            g1[...] += dot_tn(xt, dh1_s[at, :])
            g3[...] += dot_tn(xt, dh3_s[at, :])
            g2[...] += dot_tn(act_s[at, :], dyd_s[at, :])
            return c

        lax.fori_loop(0, x_steps, step, 0)

    class Sums:
        STEPS = 2 * SIDE

        def __init__(self, m):
            self.m = m

        def where(self, i):
            half = lax.rem(i, 2)
            off = pick(i // 2, PART_ORDER)
            place = jnp.where(half == 0, lax.rem(p.y + off, SIDE), lax.rem(p.x + off, SIDE))
            return half, off, place

        def arrive(self, i):
            half, off, place = self.where(i)
            for s in range(SIDE):
                for w in (0, 1):
                    ref = lined.at[self.m, half, place, s, pl.ds(w * capacity, capacity)]
                    pltpu.make_async_remote_copy(src_ref=ref, dst_ref=ref, send_sem=r_ssem.at[0, 0], recv_sem=r_rsem.at[self.m, half, place, s * 2 + w],
                                                 device_id={'ep': p.partner}, device_id_type=MESH).wait_recv()

        def load(self, i):
            half, off, place = self.where(i)
            slot = lax.rem(i, 2)
            return pltpu.make_async_copy(lined.at[self.m, half, place], line_t.at[slot], l_sem.at[slot])

        def copy(self, i):
            half, off, place = self.where(i)
            chip = jnp.where(half == 0, place * SIDE + p.x, p.y * SIDE + place)
            mine = jnp.where(half == 0, p.y, p.x)
            return pltpu.make_async_remote_copy(src_ref=sum_s.at[self.m, i], dst_ref=parts.at[self.m, half, mine], send_sem=p_ssem.at[self.m, i],
                                                recv_sem=p_rsem.at[self.m, half, mine], device_id={'ep': chip * 2 + p.core}, device_id_type=MESH)

        def run(self):
            last = self.STEPS - 2
            self.arrive(0)
            self.load(0).start()

            def step(i, c):
                @pl.when(i + 1 < self.STEPS)
                def _():
                    self.arrive(i + 1)
                    self.load(i + 1).start()
                self.load(i).wait()

                @pl.when(jnp.logical_and(i >= 1, i <= last))
                def _():
                    self.copy(i - 1).start()

                half, off, place = self.where(i)
                home = jnp.where(half == 0, place, SIDE + place)
                slot = lax.rem(i, 2)
                total = None
                for s in range(SIDE):
                    chip = jnp.where(half == 0, p.y * SIDE + s, s * SIDE + p.x)
                    want = lax.broadcasted_iota(jnp.int32, (rows, tokens), 0) + chip * rows
                    hit = idx_all[home, self.m, 0:1, :] == want
                    for j in range(1, top_k):
                        hit = hit | (idx_all[home, self.m, j:j + 1, :] == want)
                    part = dot_tn(jnp.where(hit, 1.0, 0.0).astype(BF16), line_t[slot, s])
                    total = part if total is None else total + part
                sum_s[self.m, i] = total
                return c

            lax.fori_loop(0, self.STEPS, step, 0)

        def total(self):
            for half in (0, 1):
                for o in range(1, SIDE):
                    s = lax.rem((p.y if half == 0 else p.x) + o, SIDE)
                    ref = parts.at[self.m, half, s]
                    pltpu.make_async_remote_copy(src_ref=ref, dst_ref=ref, send_sem=p_ssem.at[0, 0], recv_sem=p_rsem.at[self.m, half, s],
                                                 device_id={'ep': p.partner}, device_id_type=MESH).wait_recv()
                    pltpu.make_async_copy(ref, part_t.at[half, o - 1], f_sem.at[half, o - 1]).start()
            for half in (0, 1):
                acc = sum_s[self.m, self.STEPS - 2 + half]
                for o in range(1, SIDE):
                    pltpu.make_async_copy(parts.at[self.m, half, 0], part_t.at[half, o - 1], f_sem.at[half, o - 1]).wait()
                    acc = acc + part_t[half, o - 1]
                dx_out[self.m, :, half * wide:(half + 1) * wide] = acc.astype(BF16)

        def finish(self):
            for i in range(self.STEPS - 2):
                self.copy(i).wait_send()

    a, b = gathers
    events = {i: [] for i in range(-1, UNITS)}
    events[-1] += [lambda: a.first(0), lambda: a.first(1), lambda: a.second(0, 0), lambda: a.second(1, 0), b.begin]
    events[0] += [lambda: a.first_far(0), lambda: a.first_far(1)]
    events[1] += [lambda: a.second(0, 1), lambda: a.second(1, 1)]
    events[2] += [lambda: a.second(0, -1), lambda: a.second(1, -1)]
    events[4] += [lambda: a.second(0, 2), lambda: a.second(1, 2)]
    events[5] += [lambda: b.first(0), lambda: b.first(1)]
    events[6] += [lambda: b.second(0, 0), lambda: b.second(1, 0)]
    events[8] += [lambda: a.second_far(0)]
    events[9] += [lambda: b.first_far(0), lambda: b.first_far(1)]
    events[10] += [lambda: a.second_far(1), lambda: a.second_far(-1), lambda: a.second_far(2)]
    events[11] += [lambda: b.second(0, 1), lambda: b.second(1, 1)]
    events[12] += [lambda: b.second(0, -1), lambda: b.second(1, -1)]
    events[14] += [lambda: b.second(0, 2), lambda: b.second(1, 2)]
    for k, (ox, oy) in enumerate(ORDER):
        events[k - 1].append(functools.partial(a.from_partner, ox, oy))
    later = {1: [lambda: b.second_far(0)], 3: [lambda: b.second_far(1), lambda: b.second_far(-1)], 5: [lambda: b.second_far(2)]}

    for e in events[-1]:
        e()
    for g in (g1, g3, g2):
        g[...] = jnp.zeros_like(g)

    def recv_map(k, c):
        s = lax.rem(me + k, group)
        map_copy(s, s, k, s).wait()
        return c

    lax.fori_loop(1, group, recv_map, 0)
    own[0].wait()
    for c in weights:
        c.wait()
    units = (Units(0, ORDER), Units(1, FAR_FIRST))
    sums = (Sums(0), Sums(1))
    units[0].run(events)
    weight_grads(0, later)
    for ox, oy in ORDER:
        b.from_partner(ox, oy)
    own[1].wait()
    units[1].run({})
    for half in (0, 1):
        for o in range(1, SIDE):
            idx_wait(half, o)
    sums[0].run()
    weight_grads(1, {})
    outs = [pltpu.make_async_copy(s, t, g_sem.at[k]) for k, (s, t) in enumerate(((g1, g1_out), (g3, g3_out), (g2, g2_out)))]
    for c in outs:
        c.start()
    sums[1].run()
    for t in sums:
        t.total()

    for g in gathers:
        g.finish()
    for half in (0, 1):
        for o in range(1, SIDE):
            idx_copy(half, o).wait_send()
    for t in units + sums:
        t.finish()
    for c in outs:
        c.wait()


def START(copy):
    copy.start()


def WAIT_SEND(copy):
    copy.wait_send()


def layer_call(group, dy, topk, slots, gates, yd, x, h1, h3, w1, w3, w2):
    n_micro, tokens, d = dy.shape
    f = h1.shape[2]
    top_k = topk.shape[1]
    rows = h1.shape[1] // UNITS
    saved = h1.shape[1]
    hbm = pl.BlockSpec(memory_space=pltpu.HBM)
    vmem = pl.BlockSpec(memory_space=pltpu.VMEM)
    dma = pltpu.SemaphoreType.DMA
    shape = jax.ShapeDtypeStruct
    out = pl.pallas_call(
        functools.partial(layer_kernel, group),
        in_specs=[hbm, vmem, vmem, vmem] + [hbm] * 7,
        out_specs=[vmem, vmem] + [hbm] * 7,
        out_shape=[shape((n_micro, tokens, d), BF16), shape((n_micro, top_k, tokens), F32),
                   shape((d, f), F32), shape((d, f), F32), shape((f, d), F32),
                   shape((n_micro, group, tokens, d), BF16), shape((n_micro, UNITS, rows, d), BF16),
                   shape((n_micro, 2, SIDE, SIDE, rows, d // 2), BF16), shape((n_micro, 2, SIDE, tokens, d // 2), F32)],
        scratch_shapes=[pltpu.VMEM((group, 2 * n_micro, 1, tokens), F32), pltpu.VMEM((group, 2 * n_micro, 1, tokens), F32),
                        pltpu.VMEM((2 * SIDE, n_micro, top_k, tokens), jnp.int32),
                        pltpu.VMEM((d, f), BF16), pltpu.VMEM((d, f), BF16), pltpu.VMEM((f, d), BF16),
                        pltpu.VMEM((2, 2, tokens, d), BF16), pltpu.VMEM((2, rows, f), BF16), pltpu.VMEM((2, rows, f), BF16),
                        pltpu.VMEM((2, rows, d), BF16), pltpu.VMEM((2, 128) + yd.shape[1:], BF16), pltpu.VMEM(dy.shape, BF16),
                        pltpu.VMEM((2, 256, d), BF16), pltpu.VMEM((2, SIDE, rows, d // 2), BF16),
                        pltpu.VMEM((n_micro, 2 * SIDE, tokens, d // 2), F32), pltpu.VMEM((2, SIDE - 1, tokens, d // 2), F32),
                        pltpu.VMEM((saved, d), BF16), pltpu.VMEM((saved, f), BF16), pltpu.VMEM((saved, f), BF16), pltpu.VMEM((saved, f), BF16),
                        pltpu.VMEM((d, f), F32), pltpu.VMEM((d, f), F32), pltpu.VMEM((f, d), F32),
                        dma((n_micro, 80)), dma((n_micro, 80)), dma((group,)), dma((group,)), dma((2 * SIDE,)), dma((2 * SIDE,)),
                        dma((n_micro, 4 * UNITS)), dma((n_micro, 2, SIDE, 2 * SIDE)), dma((n_micro, 2 * SIDE)), dma((n_micro, 2, SIDE)),
                        dma((n_micro + 1,)), dma((3,)), dma((2, 3)), dma((2,)), dma((2,)), dma((2,)), dma((2,)), dma((2, SIDE - 1)), dma((3,))],
        compiler_params=pltpu.CompilerParams(collective_id=0, has_side_effects=True, vmem_limit_bytes=64 * 2**20 - 2**17),
        name='layer')(dy, topk, slots, gates, yd, x, h1, h3, w1, w3, w2)
    return out[:5]


def solution(mesh):
    group = mesh.shape['ep']
    tok_spec = P(None, ('dp', 'ep'))
    w_spec = P('ep')
    grad_w_spec = P(('dp', 'ep'))

    def local_step(grad_out, expert_out, gate_vals, topk_idx, slot_idx, x_dispatch, h1_pre, h3_pre, w_gate, w_up, w_down):
        n_micro, tokens, top_k, d = expert_out.shape
        turned = [jnp.swapaxes(v, 1, 2) for v in (topk_idx, slot_idx, gate_vals)]
        dx, dg, g1, g3, g2 = layer_call(
            group, grad_out, *turned, expert_out.reshape(n_micro * tokens, top_k, d),
            x_dispatch[:, 0], h1_pre[:, 0], h3_pre[:, 0], w_gate[0], w_up[0], w_down[0])
        return dx, jnp.swapaxes(dg, 1, 2), g1[None], g3[None], g2[None]

    in_specs = (tok_spec, tok_spec, tok_spec, tok_spec, tok_spec, tok_spec, tok_spec, tok_spec, w_spec, w_spec, w_spec)
    out_specs = (tok_spec, tok_spec, grad_w_spec, grad_w_spec, grad_w_spec)
    return jax.shard_map(local_step, mesh=mesh, in_specs=in_specs, out_specs=out_specs, check_vma=False)
```

```python
import functools
import jax
import jax.numpy as jnp
from jax import lax
from jax.experimental import pallas as pl
from jax.experimental.pallas import tpu as pltpu
from jax.sharding import PartitionSpec as P

F32 = jnp.float32
BF16 = jnp.bfloat16
MESH = pl.DeviceIdType.MESH
SIDE = 4
ORDER = [divmod(int(c, 16), SIDE) for c in '04c135f7d8296bea']
UNITS = len(ORDER)
FAR_FIRST = [divmod(int(c, 16), SIDE) for c in '26ea89b15d473fc0']
PART_ORDER = (2, 1, 3, 0)


def dot_nn(a, b):
    return lax.dot_general(a, b, (((1,), (0,)), ((), ())), preferred_element_type=F32)


def dot_nt(a, b):
    return lax.dot_general(a, b, (((1,), (1,)), ((), ())), preferred_element_type=F32)


def dot_tn(a, b):
    return lax.dot_general(a, b, (((0,), (0,)), ((), ())), preferred_element_type=F32)


def gather_rows(pos, gate, dy, rows):
    tokens = pos.shape[1]
    hit = lax.broadcasted_iota(jnp.int32, (rows, tokens), 0).astype(F32) == pos
    gate_col = jnp.sum(jnp.where(hit, gate, 0.0), axis=1, keepdims=True)
    onehot = jnp.where(hit, 1.0, 0.0).astype(BF16)
    return (dot_nn(onehot, dy) * gate_col).astype(BF16)


def swiglu_grads(dyd, h1, h3, w2):
    h1 = h1.astype(F32)
    h3 = h3.astype(F32)
    sig = jax.nn.sigmoid(h1)
    silu = h1 * sig
    act = (silu * h3).astype(BF16)
    da = dot_nt(dyd, w2).astype(BF16).astype(F32)
    dh1 = (da * h3 * sig * (1.0 + h1 * (1.0 - sig))).astype(BF16)
    dh3 = (da * silu).astype(BF16)
    return act, dh1, dh3


class Place:
    def __init__(self):
        self.me = lax.axis_index('ep')
        self.core = lax.rem(self.me, 2)
        self.chip = self.me // 2
        self.x = lax.rem(self.chip, SIDE)
        self.y = self.chip // SIDE
        self.partner = self.me + 1 - 2 * self.core

    def chip_at(self, ox, oy):
        return lax.rem(self.y + oy + SIDE, SIDE) * SIDE + lax.rem(self.x + ox + SIDE, SIDE)

    def dev(self, ox, oy):
        return self.chip_at(ox, oy) * 2 + self.core


def pick(k, values):
    out = jnp.int32(values[0])
    for j in range(1, len(values)):
        out = jnp.where(k == j, jnp.int32(values[j]), out)
    return out


class Gather:
    AXES = (((1, 0), (0, 1)), ((0, 1), (1, 0)))

    def __init__(self, place, src, out, ssem, rsem):
        self.p, self.src, self.out, self.ssem, self.rsem = place, src, out, ssem, rsem
        self.half = src.shape[0] // 2
        self.sent = []
        self.ids = {}

    def rows(self, h, q=None):
        if q is None:
            return (h * self.half, self.half)
        return (h * self.half + q * (self.half // 2), self.half // 2)

    def rid(self, *key):
        return self.ids.setdefault(key, len(self.ids))

    def send(self, origin, rows, to, rid, own=False):
        k = len(self.sent)
        cut = pl.ds(*rows)
        self.sent.append(rows[1])
        pltpu.make_async_remote_copy(
            src_ref=self.src.at[cut] if own else self.out.at[origin, cut],
            dst_ref=self.out.at[origin, cut],
            send_sem=self.ssem.at[k], recv_sem=self.rsem.at[rid],
            device_id={'ep': to}, device_id_type=MESH).start()

    def wait(self, rows, rid):
        ref = self.out.at[0, pl.ds(*rows)]
        pltpu.make_async_remote_copy(src_ref=ref, dst_ref=ref, send_sem=self.ssem.at[0], recv_sem=self.rsem.at[rid],
                                     device_id={'ep': self.p.partner}, device_id_type=MESH).wait_recv()

    def to_partner(self, ox, oy, rows, own=False):
        self.send(self.p.dev(ox, oy), rows, self.p.partner, self.rid('p', ox % SIDE, oy % SIDE, rows), own)

    def begin(self):
        for h in (0, 1):
            e1, e2 = self.AXES[h]
            for s in (1, -1):
                self.send(self.p.me, self.rows(h), self.p.dev(s * e1[0], s * e1[1]), self.rid('1', h, s), True)
            for s in (1, -1):
                self.send(self.p.me, self.rows(h), self.p.dev(s * e2[0], s * e2[1]), self.rid('2', h, s, 0), True)
        self.to_partner(0, 0, (0, 2 * self.half), True)

    def first(self, h):
        e1, e2 = self.AXES[h]
        for s in (1, -1):
            ox, oy = -s * e1[0], -s * e1[1]
            self.wait(self.rows(h), self.rid('1', h, s))
            o = self.p.dev(ox, oy)
            part = self.rows(h, 0 if s == 1 else 1)
            self.send(o, part, self.p.dev(s * e1[0], s * e1[1]), self.rid('1f', h, s))
            for t in (1, -1):
                self.send(o, self.rows(h), self.p.dev(t * e2[0], t * e2[1]), self.rid('2', h, t, -s))
            self.to_partner(ox, oy, self.rows(h))

    def second(self, h, j):
        e1, e2 = self.AXES[h]
        for s in (1, -1):
            ox, oy = j * e1[0] - s * e2[0], j * e1[1] - s * e2[1]
            part = self.rows(h, 0 if s == 1 else 1)
            if j == 2:
                for q in (0, 1):
                    self.wait(self.rows(h, q), self.rid('2', h, s, 2, q))
            else:
                self.wait(self.rows(h), self.rid('2', h, s, j))
            self.send(self.p.dev(ox, oy), part, self.p.dev(s * e2[0], s * e2[1]), self.rid('2f', h, s, j))
            self.to_partner(ox, oy, self.rows(h))

    def first_far(self, h):
        e1, e2 = self.AXES[h]
        ox, oy = 2 * e1[0], 2 * e1[1]
        for s in (1, -1):
            q = 0 if s == 1 else 1
            self.wait(self.rows(h, q), self.rid('1f', h, s))
            for t in (1, -1):
                self.send(self.p.dev(ox, oy), self.rows(h, q), self.p.dev(t * e2[0], t * e2[1]), self.rid('2', h, t, 2, q))
        self.to_partner(ox, oy, self.rows(h))

    def second_far(self, j):
        for h in (0, 1):
            e1, e2 = self.AXES[h]
            ox, oy = j * e1[0] + 2 * e2[0], j * e1[1] + 2 * e2[1]
            for s in (1, -1):
                self.wait(self.rows(h, 0 if s == 1 else 1), self.rid('2f', h, s, j))
            self.to_partner(ox, oy, self.rows(h))

    def from_partner(self, ox, oy):
        parts = [(key[3], r) for key, r in self.ids.items() if key[:3] == ('p', ox, oy)]
        assert sum(rows[1] for rows, _ in parts) == 2 * self.half
        for rows, r in parts:
            self.wait(rows, r)

    def finish(self):
        for k, size in enumerate(self.sent):
            ref = self.out.at[0, pl.ds(0, size)]
            pltpu.make_async_remote_copy(src_ref=ref, dst_ref=ref, send_sem=self.ssem.at[k], recv_sem=self.rsem.at[0],
                                         device_id={'ep': self.p.partner}, device_id_type=MESH).wait_send()


def layer_kernel(group, dy, topk, slots, gates, yd, x, h1, h3, w1, w3, w2,
                 dx_out, dg_out, g1_out, g3_out, g2_out, everyone, staged, lined,
                 maps, maps_all, idx_all, w1_v, w3_v, w2_v, dy_t, h1_t, h3_t, dx_t, yd_t, dyo, x_t, line_t, sum_s, parts, passing,
                 dyd_s, act_s, dh1_s, dh3_s, g1, g3, g2,
                 ag_ssem, ag_rsem, m_ssem, m_rsem, i_ssem, i_rsem, r_ssem, r_rsem, p_ssem, p_rsem, q_rsem,
                 own_sem, w_sem, in_sem, st_sem, yd_sem, x_sem, l_sem, g_sem):
    p = Place()
    me = p.me
    n_micro, tokens, d = dy.shape
    top_k = topk.shape[1]
    rows = lined.shape[4]
    capacity = rows // 2
    wide = d // 2
    per_micro = rows * UNITS

    barrier = pltpu.get_barrier_semaphore()

    def greet(k, c):
        pl.semaphore_signal(barrier, inc=1, device_id={'ep': lax.rem(me + k, group)}, device_id_type=MESH)
        return c

    lax.fori_loop(1, group, greet, 0)

    weights = [pltpu.make_async_copy(a, b, w_sem.at[k]) for k, (a, b) in enumerate(((w1, w1_v), (w3, w3_v), (w2, w2_v)))]
    own = [pltpu.make_async_copy(dy.at[m], everyone.at[m, me], own_sem.at[m]) for m in range(n_micro)]
    own_dy = pltpu.make_async_copy(dy, dyo, own_sem.at[n_micro])
    own_dy.start()
    yd_tokens = yd_t.shape[1]
    yd_steps = yd.shape[0] // yd_tokens

    def yd_copy(i):
        slot = lax.rem(i, 2)
        return pltpu.make_async_copy(yd.at[pl.ds(i * yd_tokens, yd_tokens)], yd_t.at[slot], yd_sem.at[slot])

    yd_copy(0).start()

    for m in range(n_micro):
        experts = lax.broadcasted_iota(jnp.int32, (group, tokens), 0)
        pos = jnp.full((group, tokens), -1, jnp.int32)
        gate = jnp.zeros((group, tokens), F32)
        for j in range(top_k):
            same = experts == topk[m, j:j + 1, :]
            at = slots[m, j:j + 1, :]
            pos = jnp.where(same, jnp.where(at >= 0, at + p.core * capacity, -1), pos)
            gate = jnp.where(same, gates[m, j:j + 1, :], gate)
        pos = pos.astype(F32)
        for e in range(group):
            maps[e, 2 * m] = pos[e:e + 1, :]
            maps[e, 2 * m + 1] = gate[e:e + 1, :]
        mine = jnp.where(slots[m] >= 0, topk[m] * capacity + slots[m], -1)
        idx_all[p.y, m] = mine
        idx_all[SIDE + p.x, m] = mine
    maps_all[me] = maps[me]

    pl.semaphore_wait(barrier, group - 1)

    gathers = [Gather(p, dy.at[m], everyone.at[m], ag_ssem.at[m], ag_rsem.at[m]) for m in range(n_micro)]
    gathers[0].begin()

    def map_copy(to, origin, slot_s, slot_r):
        return pltpu.make_async_remote_copy(src_ref=maps.at[to], dst_ref=maps_all.at[origin], send_sem=m_ssem.at[slot_s],
                                            recv_sem=m_rsem.at[slot_r], device_id={'ep': to}, device_id_type=MESH)

    def send_map(k, c):
        to = lax.rem(me + k, group)
        map_copy(to, me, k, me).start()
        return c

    lax.fori_loop(1, group, send_map, 0)

    def idx_copy(half, o):
        at = p.y if half == 0 else SIDE + p.x
        to = p.dev(0, o) if half == 0 else p.dev(o, 0)
        return pltpu.make_async_remote_copy(src_ref=idx_all.at[at], dst_ref=idx_all.at[at], send_sem=i_ssem.at[half * SIDE + o],
                                            recv_sem=i_rsem.at[at], device_id={'ep': to}, device_id_type=MESH)

    def idx_wait(half, o):
        at = lax.rem(p.y + o, SIDE) if half == 0 else SIDE + lax.rem(p.x + o, SIDE)
        pltpu.make_async_remote_copy(src_ref=idx_all.at[at], dst_ref=idx_all.at[at], send_sem=i_ssem.at[0], recv_sem=i_rsem.at[at],
                                     device_id={'ep': p.partner}, device_id_type=MESH).wait_recv()

    for half in (0, 1):
        for o in range(1, SIDE):
            idx_copy(half, o).start()
    for c in own + weights:
        c.start()

    own_dy.wait()

    def gate_step(i, c):
        @pl.when(i + 1 < yd_steps)
        def _():
            yd_copy(i + 1).start()
        yd_copy(i).wait()
        slot = lax.rem(i, 2)
        per = tokens // yd_tokens
        m = i // per
        at = pl.ds(pl.multiple_of(lax.rem(i, per) * yd_tokens, yd_tokens), yd_tokens)
        fine = 32
        out = []
        for r0 in range(0, yd_tokens, fine):
            a = dyo[m, pl.ds(pl.multiple_of(lax.rem(i, per) * yd_tokens + r0, fine), fine), :].astype(F32)
            b = yd_t[slot, r0:r0 + fine].astype(F32)
            out.append(jnp.sum(a[:, None, :] * b, axis=-1))
        dg_out[m, :, at] = jnp.concatenate(out, axis=0).T
        return c

    lax.fori_loop(0, yd_steps, gate_step, 0)

    def chip_of(order, i):
        ox, oy = pick(i, [o[0] for o in order]), pick(i, [o[1] for o in order])
        return lax.rem(p.x + ox, SIDE), lax.rem(p.y + oy, SIDE)

    class Units:
        def __init__(self, m, order):
            self.m, self.order = m, order

        def loads(self, i):
            cx, cy = chip_of(self.order, i)
            u = cy * SIDE + cx
            slot = lax.rem(i, 2)
            cut = pl.ds(pl.multiple_of(u * rows, 16), rows)
            return [pltpu.make_async_copy(everyone.at[self.m, pl.ds(2 * u, 2)], dy_t.at[slot], in_sem.at[slot, 0]),
                    pltpu.make_async_copy(h1.at[self.m, cut], h1_t.at[slot], in_sem.at[slot, 1]),
                    pltpu.make_async_copy(h3.at[self.m, cut], h3_t.at[slot], in_sem.at[slot, 2])]

        def stage(self, i):
            cx, cy = chip_of(self.order, i)
            slot = lax.rem(i, 2)
            return pltpu.make_async_copy(dx_t.at[slot], staged.at[self.m, cy * SIDE + cx], st_sem.at[slot])

        def refs(self, i, half, w):
            cx, cy = chip_of(self.order, i)
            src = staged.at[self.m, cy * SIDE + cx, pl.ds(pl.multiple_of(w * capacity, 8), capacity), pl.ds(half * wide, wide)]
            mine = pl.ds(pl.multiple_of(p.core * capacity, 8), capacity)
            place = cy if half == 0 else cx
            came = p.x if half == 0 else p.y
            dst = lined.at[self.m, half, place, came, mine]
            sem = r_rsem.at[self.m, half, place, came * 2 + p.core]
            chip = p.y * SIDE + cx if half == 0 else cy * SIDE + p.x
            here = (cx == p.x) if half == 0 else (cy == p.y)
            return src, dst, sem, chip * 2 + w, here

        def each(self, i, act):
            for half in (0, 1):
                for w in (0, 1):
                    src, dst, sem, to, here = self.refs(i, half, w)
                    remote = pltpu.make_async_remote_copy(src_ref=src, dst_ref=dst, send_sem=r_ssem.at[self.m, i * 4 + half * 2 + w], recv_sem=sem,
                                                          device_id={'ep': to}, device_id_type=MESH)
                    self_too = jnp.logical_and(here, p.core == w)

                    @pl.when(jnp.logical_not(self_too))
                    def _():
                        act(remote)

                    if act is START:
                        @pl.when(self_too)
                        def _():
                            pltpu.make_async_copy(src, dst, sem).start()

        def run(self, events):
            for t in self.loads(0):
                t.start()

            def step(i, c):
                for k in range(UNITS):
                    if events.get(k):
                        @pl.when(i == k)
                        def _():
                            for e in events[k]:
                                e()

                @pl.when(i + 1 < UNITS)
                def _():
                    for t in self.loads(i + 1):
                        t.start()

                @pl.when(i >= 1)
                def _():
                    self.stage(i - 1).wait()
                    self.each(i - 1, START)

                for t in self.loads(i):
                    t.wait()
                m = self.m
                cx, cy = chip_of(self.order, i)
                u = cy * SIDE + cx
                slot = lax.rem(i, 2)
                pos = jnp.concatenate([maps_all[2 * u, 2 * m], maps_all[2 * u + 1, 2 * m]], axis=1)
                gate = jnp.concatenate([maps_all[2 * u, 2 * m + 1], maps_all[2 * u + 1, 2 * m + 1]], axis=1)
                dyd = gather_rows(pos, gate, dy_t[slot].reshape(2 * tokens, d), rows)
                act, dh1, dh3 = swiglu_grads(dyd, h1_t[slot], h3_t[slot], w2_v[...])
                dx_t[slot] = (dot_nt(dh1, w1_v[...]) + dot_nt(dh3, w3_v[...])).astype(BF16)
                self.stage(i).start()
                at = pl.ds(pl.multiple_of(u * rows, 16), rows)
                dyd_s[at, :] = dyd
                act_s[at, :] = act
                dh1_s[at, :] = dh1
                dh3_s[at, :] = dh3
                return c

            lax.fori_loop(0, UNITS, step, 0)
            self.stage(UNITS - 1).wait()
            self.each(UNITS - 1, START)

        def finish(self):
            def step(i, c):
                self.each(i, WAIT_SEND)
                return c
            lax.fori_loop(0, UNITS, step, 0)

    depth = x_t.shape[1]
    x_steps = per_micro // depth

    def weight_grads(m, events):
        def x_copy(i):
            slot = lax.rem(i, 2)
            return pltpu.make_async_copy(x.at[m, pl.ds(pl.multiple_of(i * depth, depth), depth)], x_t.at[slot], x_sem.at[slot])

        x_copy(0).start()

        def step(i, c):
            for k in range(x_steps):
                if events.get(k):
                    @pl.when(i == k)
                    def _():
                        for e in events[k]:
                            e()

            @pl.when(i + 1 < x_steps)
            def _():
                x_copy(i + 1).start()
            x_copy(i).wait()
            at = pl.ds(pl.multiple_of(i * depth, depth), depth)
            xt = x_t[lax.rem(i, 2)]
            g1[...] += dot_tn(xt, dh1_s[at, :])
            g3[...] += dot_tn(xt, dh3_s[at, :])
            g2[...] += dot_tn(act_s[at, :], dyd_s[at, :])
            return c

        lax.fori_loop(0, x_steps, step, 0)

    class Sums:
        STEPS = 2 * SIDE

        def __init__(self, m):
            self.m = m

        def where(self, i):
            half = lax.rem(i, 2)
            off = pick(i // 2, PART_ORDER)
            place = jnp.where(half == 0, lax.rem(p.y + off, SIDE), lax.rem(p.x + off, SIDE))
            return half, off, place

        def arrive(self, i):
            half, off, place = self.where(i)
            for s in range(SIDE):
                for w in (0, 1):
                    ref = lined.at[self.m, half, place, s, pl.ds(w * capacity, capacity)]
                    pltpu.make_async_remote_copy(src_ref=ref, dst_ref=ref, send_sem=r_ssem.at[0, 0], recv_sem=r_rsem.at[self.m, half, place, s * 2 + w],
                                                 device_id={'ep': p.partner}, device_id_type=MESH).wait_recv()

        def load(self, i):
            half, off, place = self.where(i)
            slot = lax.rem(i, 2)
            return pltpu.make_async_copy(lined.at[self.m, half, place], line_t.at[slot], l_sem.at[slot])

        def relay(self, i, half, up):
            home = lax.rem((p.x if half else p.y) + 2, SIDE)
            step = 1 if up else SIDE - 1
            to = p.dev(step, 0) if half else p.dev(0, step)
            return pltpu.make_async_remote_copy(src_ref=sum_s.at[self.m, i, pl.ds(tokens // 2 * up, tokens // 2)], dst_ref=passing.at[self.m, half, up],
                                                send_sem=p_ssem.at[self.m, i, up], recv_sem=q_rsem.at[self.m, half, up],
                                                device_id={'ep': to}, device_id_type=MESH)

        def copy(self, i, half, up):
            step = 1 if up else SIDE - 1
            to = p.dev(step, 0) if half else p.dev(0, step)
            return pltpu.make_async_remote_copy(src_ref=sum_s.at[self.m, i], dst_ref=parts.at[self.m, half, up], send_sem=p_ssem.at[self.m, i, 0],
                                                recv_sem=p_rsem.at[self.m, half, up], device_id={'ep': to}, device_id_type=MESH)

        def sends(self, i):
            half = i % 2
            if i < 2:
                return [self.relay(i, half, up) for up in (0, 1)]
            if i < self.STEPS - 2:
                return [self.copy(i, half, 1 - (i // 2 - 1))]
            return []

        def came(self, ref, sem):
            pltpu.make_async_remote_copy(src_ref=ref, dst_ref=ref, send_sem=p_ssem.at[0, 0, 0], recv_sem=sem,
                                         device_id={'ep': p.partner}, device_id_type=MESH).wait_recv()

        def run(self):
            self.arrive(0)
            self.load(0).start()

            def step(i, c):
                @pl.when(i + 1 < self.STEPS)
                def _():
                    self.arrive(i + 1)
                    self.load(i + 1).start()
                self.load(i).wait()

                for k in range(1, self.STEPS - 1):
                    @pl.when(i == k)
                    def _():
                        for t in self.sends(k - 1):
                            t.start()

                half, off, place = self.where(i)
                home = jnp.where(half == 0, place, SIDE + place)
                slot = lax.rem(i, 2)
                total = None
                for s in range(SIDE):
                    chip = jnp.where(half == 0, p.y * SIDE + s, s * SIDE + p.x)
                    want = lax.broadcasted_iota(jnp.int32, (rows, tokens), 0) + chip * rows
                    hit = idx_all[home, self.m, 0:1, :] == want
                    for j in range(1, top_k):
                        hit = hit | (idx_all[home, self.m, j:j + 1, :] == want)
                    part = dot_tn(jnp.where(hit, 1.0, 0.0).astype(BF16), line_t[slot, s])
                    total = part if total is None else total + part
                sum_s[self.m, i] = total
                for k in range(2, self.STEPS - 2):
                    @pl.when(i == k)
                    def _():
                        up = 1 - (k // 2 - 1)
                        ref = passing.at[self.m, k % 2, up]
                        self.came(ref, q_rsem.at[self.m, k % 2, up])
                        cut = pl.ds(tokens // 2 * up, tokens // 2)
                        sum_s[self.m, k, cut] = sum_s[self.m, k, cut] + passing[self.m, k % 2, up]
                return c

            lax.fori_loop(0, self.STEPS, step, 0)

        def total(self):
            for half in (0, 1):
                acc = sum_s[self.m, self.STEPS - 2 + half]
                for up in (0, 1):
                    self.came(parts.at[self.m, half, up], p_rsem.at[self.m, half, up])
                    acc = acc + parts[self.m, half, up]
                dx_out[self.m, :, half * wide:(half + 1) * wide] = acc.astype(BF16)

        def finish(self):
            for i in range(self.STEPS):
                for t in self.sends(i):
                    t.wait_send()

    a, b = gathers
    events = {i: [] for i in range(-1, UNITS)}
    events[-1] += [lambda: a.first(0), lambda: a.first(1), lambda: a.second(0, 0), lambda: a.second(1, 0), b.begin]
    events[0] += [lambda: a.first_far(0), lambda: a.first_far(1)]
    events[1] += [lambda: a.second(0, 1), lambda: a.second(1, 1)]
    events[2] += [lambda: a.second(0, -1), lambda: a.second(1, -1)]
    events[4] += [lambda: a.second(0, 2), lambda: a.second(1, 2)]
    events[5] += [lambda: b.first(0), lambda: b.first(1)]
    events[6] += [lambda: b.second(0, 0), lambda: b.second(1, 0)]
    events[8] += [lambda: a.second_far(0)]
    events[9] += [lambda: b.first_far(0), lambda: b.first_far(1)]
    events[10] += [lambda: a.second_far(1), lambda: a.second_far(-1), lambda: a.second_far(2)]
    events[11] += [lambda: b.second(0, 1), lambda: b.second(1, 1)]
    events[12] += [lambda: b.second(0, -1), lambda: b.second(1, -1)]
    events[14] += [lambda: b.second(0, 2), lambda: b.second(1, 2)]
    for k, (ox, oy) in enumerate(ORDER):
        events[k - 1].append(functools.partial(a.from_partner, ox, oy))
    later = {1: [lambda: b.second_far(0)], 3: [lambda: b.second_far(1), lambda: b.second_far(-1)], 5: [lambda: b.second_far(2)]}

    for e in events[-1]:
        e()
    for g in (g1, g3, g2):
        g[...] = jnp.zeros_like(g)

    def recv_map(k, c):
        s = lax.rem(me + k, group)
        map_copy(s, s, k, s).wait()
        return c

    lax.fori_loop(1, group, recv_map, 0)
    own[0].wait()
    for c in weights:
        c.wait()
    units = (Units(0, ORDER), Units(1, FAR_FIRST))
    sums = (Sums(0), Sums(1))
    units[0].run(events)
    weight_grads(0, later)
    for ox, oy in ORDER:
        b.from_partner(ox, oy)
    own[1].wait()
    units[1].run({})
    for half in (0, 1):
        for o in range(1, SIDE):
            idx_wait(half, o)
    sums[0].run()
    weight_grads(1, {})
    outs = [pltpu.make_async_copy(s, t, g_sem.at[k]) for k, (s, t) in enumerate(((g1, g1_out), (g3, g3_out), (g2, g2_out)))]
    for c in outs:
        c.start()
    sums[1].run()
    for t in sums:
        t.total()

    for g in gathers:
        g.finish()
    for half in (0, 1):
        for o in range(1, SIDE):
            idx_copy(half, o).wait_send()
    for t in units + sums:
        t.finish()
    for c in outs:
        c.wait()


def START(copy):
    copy.start()


def WAIT_SEND(copy):
    copy.wait_send()


def layer_call(group, dy, topk, slots, gates, yd, x, h1, h3, w1, w3, w2):
    n_micro, tokens, d = dy.shape
    f = h1.shape[2]
    top_k = topk.shape[1]
    rows = h1.shape[1] // UNITS
    saved = h1.shape[1]
    hbm = pl.BlockSpec(memory_space=pltpu.HBM)
    vmem = pl.BlockSpec(memory_space=pltpu.VMEM)
    dma = pltpu.SemaphoreType.DMA
    shape = jax.ShapeDtypeStruct
    out = pl.pallas_call(
        functools.partial(layer_kernel, group),
        in_specs=[hbm, vmem, vmem, vmem] + [hbm] * 7,
        out_specs=[vmem, vmem] + [hbm] * 6,
        out_shape=[shape((n_micro, tokens, d), BF16), shape((n_micro, top_k, tokens), F32),
                   shape((d, f), F32), shape((d, f), F32), shape((f, d), F32),
                   shape((n_micro, group, tokens, d), BF16), shape((n_micro, UNITS, rows, d), BF16),
                   shape((n_micro, 2, SIDE, SIDE, rows, d // 2), BF16)],
        scratch_shapes=[pltpu.VMEM((group, 2 * n_micro, 1, tokens), F32), pltpu.VMEM((group, 2 * n_micro, 1, tokens), F32),
                        pltpu.VMEM((2 * SIDE, n_micro, top_k, tokens), jnp.int32),
                        pltpu.VMEM((d, f), BF16), pltpu.VMEM((d, f), BF16), pltpu.VMEM((f, d), BF16),
                        pltpu.VMEM((2, 2, tokens, d), BF16), pltpu.VMEM((2, rows, f), BF16), pltpu.VMEM((2, rows, f), BF16),
                        pltpu.VMEM((2, rows, d), BF16), pltpu.VMEM((2, 128) + yd.shape[1:], BF16), pltpu.VMEM(dy.shape, BF16),
                        pltpu.VMEM((2, 256, d), BF16), pltpu.VMEM((2, SIDE, rows, d // 2), BF16),
                        pltpu.VMEM((n_micro, 2 * SIDE, tokens, d // 2), F32), pltpu.VMEM((n_micro, 2, 2, tokens, d // 2), F32), pltpu.VMEM((n_micro, 2, 2, tokens // 2, d // 2), F32),
                        pltpu.VMEM((saved, d), BF16), pltpu.VMEM((saved, f), BF16), pltpu.VMEM((saved, f), BF16), pltpu.VMEM((saved, f), BF16),
                        pltpu.VMEM((d, f), F32), pltpu.VMEM((d, f), F32), pltpu.VMEM((f, d), F32),
                        dma((n_micro, 80)), dma((n_micro, 80)), dma((group,)), dma((group,)), dma((2 * SIDE,)), dma((2 * SIDE,)),
                        dma((n_micro, 4 * UNITS)), dma((n_micro, 2, SIDE, 2 * SIDE)), dma((n_micro, 2 * SIDE, 2)), dma((n_micro, 2, 2)), dma((n_micro, 2, 2)),
                        dma((n_micro + 1,)), dma((3,)), dma((2, 3)), dma((2,)), dma((2,)), dma((2,)), dma((2,)), dma((3,))],
        compiler_params=pltpu.CompilerParams(collective_id=0, has_side_effects=True, vmem_limit_bytes=64 * 2**20 - 2**17),
        name='layer')(dy, topk, slots, gates, yd, x, h1, h3, w1, w3, w2)
    return out[:5]


def pass_on_kernel(n, cuts, *refs):
    src, dst, held, (sem_in, sem_out) = refs[:n], refs[n:2 * n], refs[2 * n:3 * n], refs[3 * n:]
    jobs = []
    for a in range(n):
        size = src[a].shape[0] // cuts[a]
        for k in range(cuts[a]):
            at = pl.ds(k * size, size)
            jobs.append((src[a].at[at], held[a].at[at], dst[a].at[at]))
    moves = [(pltpu.make_async_copy(s, h, sem_in.at[k]), pltpu.make_async_copy(h, t, sem_out.at[k])) for k, (s, h, t) in enumerate(jobs)]
    for load, store in moves:
        load.start()
    for load, store in moves:
        load.wait()
        store.start()
    for load, store in moves:
        store.wait()


def pass_on(values, cuts):
    hbm = pl.BlockSpec(memory_space=pltpu.HBM)
    n = len(values)
    jobs = sum(cuts)
    return pl.pallas_call(
        functools.partial(pass_on_kernel, n, cuts),
        in_specs=[hbm] * n, out_specs=[hbm] * n,
        out_shape=[jax.ShapeDtypeStruct(v.shape, v.dtype) for v in values],
        scratch_shapes=[pltpu.VMEM(v.shape, v.dtype) for v in values] + [pltpu.SemaphoreType.DMA((jobs,)), pltpu.SemaphoreType.DMA((jobs,))],
        compiler_params=pltpu.CompilerParams(vmem_limit_bytes=64 * 2**20 - 2**17),
        name='pass_on')(*values)


def solution(mesh):
    group = mesh.shape['ep']
    tok_spec = P(None, ('dp', 'ep'))
    w_spec = P('ep')
    grad_w_spec = P(('dp', 'ep'))

    def local_step(grad_out, expert_out, gate_vals, topk_idx, slot_idx, x_dispatch, h1_pre, h3_pre, w_gate, w_up, w_down):
        n_micro, tokens, top_k, d = expert_out.shape
        turned = [jnp.swapaxes(v, 1, 2) for v in (topk_idx, slot_idx, gate_vals)]
        dx, dg, g1, g3, g2 = layer_call(
            group, grad_out, *turned, expert_out.reshape(n_micro * tokens, top_k, d),
            x_dispatch[:, 0], h1_pre[:, 0], h3_pre[:, 0], w_gate[0], w_up[0], w_down[0])
        dx, dg, g1, g3, g2 = pass_on((dx, dg, g1, g3, g2), (n_micro, 1, 4, 4, 4))
        return dx, jnp.swapaxes(dg, 1, 2), g1[None], g3[None], g2[None]

    in_specs = (tok_spec, tok_spec, tok_spec, tok_spec, tok_spec, tok_spec, tok_spec, tok_spec, w_spec, w_spec, w_spec)
    out_specs = (tok_spec, tok_spec, grad_w_spec, grad_w_spec, grad_w_spec)
    return jax.shard_map(local_step, mesh=mesh, in_specs=in_specs, out_specs=out_specs, check_vma=False)
```

```python
import functools
import jax
import jax.numpy as jnp
from jax import lax
from jax.experimental import pallas as pl
from jax.experimental.pallas import tpu as pltpu
from jax.sharding import PartitionSpec as P

F32 = jnp.float32
BF16 = jnp.bfloat16
MESH = pl.DeviceIdType.MESH
SIDE = 4
ORDER = [divmod(int(c, 16), SIDE) for c in '04c135f7d8296bea']
UNITS = len(ORDER)
FAR_FIRST = [divmod(int(c, 16), SIDE) for c in '26ea89b15d473fc0']
PART_ORDER = (2, 1, 3, 0)


def dot_nn(a, b):
    return lax.dot_general(a, b, (((1,), (0,)), ((), ())), preferred_element_type=F32)


def dot_nt(a, b):
    return lax.dot_general(a, b, (((1,), (1,)), ((), ())), preferred_element_type=F32)


def dot_tn(a, b):
    return lax.dot_general(a, b, (((0,), (0,)), ((), ())), preferred_element_type=F32)


def gather_rows(pos, gate, dy, rows):
    tokens = pos.shape[1]
    hit = lax.broadcasted_iota(jnp.int32, (rows, tokens), 0).astype(F32) == pos
    gate_col = jnp.sum(jnp.where(hit, gate, 0.0), axis=1, keepdims=True)
    onehot = jnp.where(hit, 1.0, 0.0).astype(BF16)
    return (dot_nn(onehot, dy) * gate_col).astype(BF16)


def swiglu_grads(dyd, h1, h3, w2):
    h1 = h1.astype(F32)
    h3 = h3.astype(F32)
    sig = jax.nn.sigmoid(h1)
    silu = h1 * sig
    act = (silu * h3).astype(BF16)
    da = dot_nt(dyd, w2).astype(BF16).astype(F32)
    dh1 = (da * h3 * sig * (1.0 + h1 * (1.0 - sig))).astype(BF16)
    dh3 = (da * silu).astype(BF16)
    return act, dh1, dh3


class Place:
    def __init__(self):
        self.me = lax.axis_index('ep')
        self.core = lax.rem(self.me, 2)
        self.chip = self.me // 2
        self.x = lax.rem(self.chip, SIDE)
        self.y = self.chip // SIDE
        self.partner = self.me + 1 - 2 * self.core

    def chip_at(self, ox, oy):
        return lax.rem(self.y + oy + SIDE, SIDE) * SIDE + lax.rem(self.x + ox + SIDE, SIDE)

    def dev(self, ox, oy):
        return self.chip_at(ox, oy) * 2 + self.core


def pick(k, values):
    out = jnp.int32(values[0])
    for j in range(1, len(values)):
        out = jnp.where(k == j, jnp.int32(values[j]), out)
    return out


class Gather:
    AXES = (((1, 0), (0, 1)), ((0, 1), (1, 0)))

    def __init__(self, place, src, out, ssem, rsem):
        self.p, self.src, self.out, self.ssem, self.rsem = place, src, out, ssem, rsem
        self.half = src.shape[0] // 2
        self.sent = []
        self.ids = {}

    def rows(self, h, q=None):
        if q is None:
            return (h * self.half, self.half)
        return (h * self.half + q * (self.half // 2), self.half // 2)

    def rid(self, *key):
        return self.ids.setdefault(key, len(self.ids))

    def send(self, origin, rows, to, rid, own=False):
        k = len(self.sent)
        cut = pl.ds(*rows)
        self.sent.append(rows[1])
        pltpu.make_async_remote_copy(
            src_ref=self.src.at[cut] if own else self.out.at[origin, cut],
            dst_ref=self.out.at[origin, cut],
            send_sem=self.ssem.at[k], recv_sem=self.rsem.at[rid],
            device_id={'ep': to}, device_id_type=MESH).start()

    def wait(self, rows, rid):
        ref = self.out.at[0, pl.ds(*rows)]
        pltpu.make_async_remote_copy(src_ref=ref, dst_ref=ref, send_sem=self.ssem.at[0], recv_sem=self.rsem.at[rid],
                                     device_id={'ep': self.p.partner}, device_id_type=MESH).wait_recv()

    def to_partner(self, ox, oy, rows, own=False):
        self.send(self.p.dev(ox, oy), rows, self.p.partner, self.rid('p', ox % SIDE, oy % SIDE, rows), own)

    def begin(self):
        for h in (0, 1):
            e1, e2 = self.AXES[h]
            for s in (1, -1):
                self.send(self.p.me, self.rows(h), self.p.dev(s * e1[0], s * e1[1]), self.rid('1', h, s), True)
            for s in (1, -1):
                self.send(self.p.me, self.rows(h), self.p.dev(s * e2[0], s * e2[1]), self.rid('2', h, s, 0), True)
        self.to_partner(0, 0, (0, 2 * self.half), True)

    def first(self, h):
        e1, e2 = self.AXES[h]
        for s in (1, -1):
            ox, oy = -s * e1[0], -s * e1[1]
            self.wait(self.rows(h), self.rid('1', h, s))
            o = self.p.dev(ox, oy)
            part = self.rows(h, 0 if s == 1 else 1)
            self.send(o, part, self.p.dev(s * e1[0], s * e1[1]), self.rid('1f', h, s))
            for t in (1, -1):
                self.send(o, self.rows(h), self.p.dev(t * e2[0], t * e2[1]), self.rid('2', h, t, -s))
            self.to_partner(ox, oy, self.rows(h))

    def second(self, h, j):
        e1, e2 = self.AXES[h]
        for s in (1, -1):
            ox, oy = j * e1[0] - s * e2[0], j * e1[1] - s * e2[1]
            part = self.rows(h, 0 if s == 1 else 1)
            if j == 2:
                for q in (0, 1):
                    self.wait(self.rows(h, q), self.rid('2', h, s, 2, q))
            else:
                self.wait(self.rows(h), self.rid('2', h, s, j))
            self.send(self.p.dev(ox, oy), part, self.p.dev(s * e2[0], s * e2[1]), self.rid('2f', h, s, j))
            self.to_partner(ox, oy, self.rows(h))

    def first_far(self, h):
        e1, e2 = self.AXES[h]
        ox, oy = 2 * e1[0], 2 * e1[1]
        for s in (1, -1):
            q = 0 if s == 1 else 1
            self.wait(self.rows(h, q), self.rid('1f', h, s))
            for t in (1, -1):
                self.send(self.p.dev(ox, oy), self.rows(h, q), self.p.dev(t * e2[0], t * e2[1]), self.rid('2', h, t, 2, q))
        self.to_partner(ox, oy, self.rows(h))

    def second_far(self, j):
        for h in (0, 1):
            e1, e2 = self.AXES[h]
            ox, oy = j * e1[0] + 2 * e2[0], j * e1[1] + 2 * e2[1]
            for s in (1, -1):
                self.wait(self.rows(h, 0 if s == 1 else 1), self.rid('2f', h, s, j))
            self.to_partner(ox, oy, self.rows(h))

    def from_partner(self, ox, oy):
        parts = [(key[3], r) for key, r in self.ids.items() if key[:3] == ('p', ox, oy)]
        assert sum(rows[1] for rows, _ in parts) == 2 * self.half
        for rows, r in parts:
            self.wait(rows, r)

    def finish(self):
        for k, size in enumerate(self.sent):
            ref = self.out.at[0, pl.ds(0, size)]
            pltpu.make_async_remote_copy(src_ref=ref, dst_ref=ref, send_sem=self.ssem.at[k], recv_sem=self.rsem.at[0],
                                         device_id={'ep': self.p.partner}, device_id_type=MESH).wait_send()


def layer_kernel(group, dy, topk, slots, gates, yd, x, h1, h3, w1, w3, w2,
                 dx_out, dg_out, g1_out, g3_out, g2_out, everyone, staged, lined,
                 maps, maps_all, idx_all, w1_v, w3_v, w2_v, dy_t, h1_t, h3_t, dx_t, yd_t, dyo, x_t, line_t, sum_s, parts, passing,
                 dyd_s, act_s, dh1_s, dh3_s, g1, g3, g2,
                 ag_ssem, ag_rsem, m_ssem, m_rsem, i_ssem, i_rsem, r_ssem, r_rsem, p_ssem, p_rsem, q_rsem,
                 own_sem, w_sem, in_sem, st_sem, yd_sem, x_sem, l_sem, g_sem):
    p = Place()
    me = p.me
    n_micro, tokens, d = dy.shape
    top_k = topk.shape[1]
    rows = lined.shape[4]
    capacity = rows // 2
    wide = d // 2
    per_micro = rows * UNITS

    barrier = pltpu.get_barrier_semaphore()

    def greet(k, c):
        pl.semaphore_signal(barrier, inc=1, device_id={'ep': lax.rem(me + k, group)}, device_id_type=MESH)
        return c

    lax.fori_loop(1, group, greet, 0)

    weights = [pltpu.make_async_copy(a, b, w_sem.at[k]) for k, (a, b) in enumerate(((w1, w1_v), (w3, w3_v), (w2, w2_v)))]
    own = [pltpu.make_async_copy(dy.at[m], everyone.at[m, me], own_sem.at[m]) for m in range(n_micro)]
    own_dy = pltpu.make_async_copy(dy, dyo, own_sem.at[n_micro])
    own_dy.start()
    yd_tokens = yd_t.shape[1]
    yd_steps = yd.shape[0] // yd_tokens

    def yd_copy(i):
        slot = lax.rem(i, 2)
        return pltpu.make_async_copy(yd.at[pl.ds(i * yd_tokens, yd_tokens)], yd_t.at[slot], yd_sem.at[slot])

    yd_copy(0).start()

    for m in range(n_micro):
        experts = lax.broadcasted_iota(jnp.int32, (group, tokens), 0)
        pos = jnp.full((group, tokens), -1, jnp.int32)
        gate = jnp.zeros((group, tokens), F32)
        for j in range(top_k):
            same = experts == topk[m, j:j + 1, :]
            at = slots[m, j:j + 1, :]
            pos = jnp.where(same, jnp.where(at >= 0, at + p.core * capacity, -1), pos)
            gate = jnp.where(same, gates[m, j:j + 1, :], gate)
        pos = pos.astype(F32)
        for e in range(group):
            maps[e, 2 * m] = pos[e:e + 1, :]
            maps[e, 2 * m + 1] = gate[e:e + 1, :]
        mine = jnp.where(slots[m] >= 0, topk[m] * capacity + slots[m], -1)
        idx_all[p.y, m] = mine
        idx_all[SIDE + p.x, m] = mine
    maps_all[me] = maps[me]

    pl.semaphore_wait(barrier, group - 1)

    gathers = [Gather(p, dy.at[m], everyone.at[m], ag_ssem.at[m], ag_rsem.at[m]) for m in range(n_micro)]
    gathers[0].begin()

    def map_copy(to, origin, slot_s, slot_r):
        return pltpu.make_async_remote_copy(src_ref=maps.at[to], dst_ref=maps_all.at[origin], send_sem=m_ssem.at[slot_s],
                                            recv_sem=m_rsem.at[slot_r], device_id={'ep': to}, device_id_type=MESH)

    def send_map(k, c):
        to = lax.rem(me + k, group)
        map_copy(to, me, k, me).start()
        return c

    lax.fori_loop(1, group, send_map, 0)

    def idx_copy(half, o):
        at = p.y if half == 0 else SIDE + p.x
        to = p.dev(0, o) if half == 0 else p.dev(o, 0)
        return pltpu.make_async_remote_copy(src_ref=idx_all.at[at], dst_ref=idx_all.at[at], send_sem=i_ssem.at[half * SIDE + o],
                                            recv_sem=i_rsem.at[at], device_id={'ep': to}, device_id_type=MESH)

    def idx_wait(half, o):
        at = lax.rem(p.y + o, SIDE) if half == 0 else SIDE + lax.rem(p.x + o, SIDE)
        pltpu.make_async_remote_copy(src_ref=idx_all.at[at], dst_ref=idx_all.at[at], send_sem=i_ssem.at[0], recv_sem=i_rsem.at[at],
                                     device_id={'ep': p.partner}, device_id_type=MESH).wait_recv()

    for half in (0, 1):
        for o in range(1, SIDE):
            idx_copy(half, o).start()
    for c in own + weights:
        c.start()

    own_dy.wait()

    def gate_step(i, c):
        @pl.when(i + 1 < yd_steps)
        def _():
            yd_copy(i + 1).start()
        yd_copy(i).wait()
        slot = lax.rem(i, 2)
        per = tokens // yd_tokens
        m = i // per
        at = pl.ds(pl.multiple_of(lax.rem(i, per) * yd_tokens, yd_tokens), yd_tokens)
        fine = 32
        out = []
        for r0 in range(0, yd_tokens, fine):
            a = dyo[m, pl.ds(pl.multiple_of(lax.rem(i, per) * yd_tokens + r0, fine), fine), :].astype(F32)
            b = yd_t[slot, r0:r0 + fine].astype(F32)
            out.append(jnp.sum(a[:, None, :] * b, axis=-1))
        dg_out[m, :, at] = jnp.concatenate(out, axis=0).T
        return c

    lax.fori_loop(0, yd_steps, gate_step, 0)

    def chip_of(order, i):
        ox, oy = pick(i, [o[0] for o in order]), pick(i, [o[1] for o in order])
        return lax.rem(p.x + ox, SIDE), lax.rem(p.y + oy, SIDE)

    class Units:
        def __init__(self, m, order):
            self.m, self.order = m, order

        def loads(self, i):
            cx, cy = chip_of(self.order, i)
            u = cy * SIDE + cx
            slot = lax.rem(i, 2)
            cut = pl.ds(pl.multiple_of(u * rows, 16), rows)
            return [pltpu.make_async_copy(everyone.at[self.m, pl.ds(2 * u, 2)], dy_t.at[slot], in_sem.at[slot, 0]),
                    pltpu.make_async_copy(h1.at[self.m, cut], h1_t.at[slot], in_sem.at[slot, 1]),
                    pltpu.make_async_copy(h3.at[self.m, cut], h3_t.at[slot], in_sem.at[slot, 2])]

        def stage(self, i):
            cx, cy = chip_of(self.order, i)
            slot = lax.rem(i, 2)
            return pltpu.make_async_copy(dx_t.at[slot], staged.at[self.m, cy * SIDE + cx], st_sem.at[slot])

        def refs(self, i, half, w):
            cx, cy = chip_of(self.order, i)
            src = staged.at[self.m, cy * SIDE + cx, pl.ds(pl.multiple_of(w * capacity, 8), capacity), pl.ds(half * wide, wide)]
            mine = pl.ds(pl.multiple_of(p.core * capacity, 8), capacity)
            place = cy if half == 0 else cx
            came = p.x if half == 0 else p.y
            dst = lined.at[self.m, half, place, came, mine]
            sem = r_rsem.at[self.m, half, place, came * 2 + p.core]
            chip = p.y * SIDE + cx if half == 0 else cy * SIDE + p.x
            here = (cx == p.x) if half == 0 else (cy == p.y)
            return src, dst, sem, chip * 2 + w, here

        def each(self, i, act):
            for half in (0, 1):
                for w in (0, 1):
                    src, dst, sem, to, here = self.refs(i, half, w)
                    remote = pltpu.make_async_remote_copy(src_ref=src, dst_ref=dst, send_sem=r_ssem.at[self.m, i * 4 + half * 2 + w], recv_sem=sem,
                                                          device_id={'ep': to}, device_id_type=MESH)
                    self_too = jnp.logical_and(here, p.core == w)

                    @pl.when(jnp.logical_not(self_too))
                    def _():
                        act(remote)

                    if act is START:
                        @pl.when(self_too)
                        def _():
                            pltpu.make_async_copy(src, dst, sem).start()

        def run(self, events):
            for t in self.loads(0):
                t.start()

            def step(i, c):
                for k in range(UNITS):
                    if events.get(k):
                        @pl.when(i == k)
                        def _():
                            for e in events[k]:
                                e()

                @pl.when(i + 1 < UNITS)
                def _():
                    for t in self.loads(i + 1):
                        t.start()

                @pl.when(i >= 1)
                def _():
                    self.stage(i - 1).wait()
                    self.each(i - 1, START)

                for t in self.loads(i):
                    t.wait()
                m = self.m
                cx, cy = chip_of(self.order, i)
                u = cy * SIDE + cx
                slot = lax.rem(i, 2)
                pos = jnp.concatenate([maps_all[2 * u, 2 * m], maps_all[2 * u + 1, 2 * m]], axis=1)
                gate = jnp.concatenate([maps_all[2 * u, 2 * m + 1], maps_all[2 * u + 1, 2 * m + 1]], axis=1)
                dyd = gather_rows(pos, gate, dy_t[slot].reshape(2 * tokens, d), rows)
                act, dh1, dh3 = swiglu_grads(dyd, h1_t[slot], h3_t[slot], w2_v[...])
                dx_t[slot] = (dot_nt(dh1, w1_v[...]) + dot_nt(dh3, w3_v[...])).astype(BF16)
                self.stage(i).start()
                at = pl.ds(pl.multiple_of(u * rows, 16), rows)
                dyd_s[at, :] = dyd
                act_s[at, :] = act
                dh1_s[at, :] = dh1
                dh3_s[at, :] = dh3
                return c

            lax.fori_loop(0, UNITS, step, 0)
            self.stage(UNITS - 1).wait()
            self.each(UNITS - 1, START)

        def finish(self):
            def step(i, c):
                self.each(i, WAIT_SEND)
                return c
            lax.fori_loop(0, UNITS, step, 0)

    depth = x_t.shape[1]
    x_steps = per_micro // depth

    def weight_grads(m, events):
        def x_copy(i):
            slot = lax.rem(i, 2)
            return pltpu.make_async_copy(x.at[m, pl.ds(pl.multiple_of(i * depth, depth), depth)], x_t.at[slot], x_sem.at[slot])

        x_copy(0).start()

        def step(i, c):
            for k in range(x_steps):
                if events.get(k):
                    @pl.when(i == k)
                    def _():
                        for e in events[k]:
                            e()

            @pl.when(i + 1 < x_steps)
            def _():
                x_copy(i + 1).start()
            x_copy(i).wait()
            at = pl.ds(pl.multiple_of(i * depth, depth), depth)
            xt = x_t[lax.rem(i, 2)]
            g1[...] += dot_tn(xt, dh1_s[at, :])
            g3[...] += dot_tn(xt, dh3_s[at, :])
            g2[...] += dot_tn(act_s[at, :], dyd_s[at, :])
            return c

        lax.fori_loop(0, x_steps, step, 0)

    class Sums:
        STEPS = 2 * SIDE

        def __init__(self, m):
            self.m = m

        def where(self, i):
            half = lax.rem(i, 2)
            off = pick(i // 2, PART_ORDER)
            place = jnp.where(half == 0, lax.rem(p.y + off, SIDE), lax.rem(p.x + off, SIDE))
            return half, off, place

        def arrive(self, i):
            half, off, place = self.where(i)
            for s in range(SIDE):
                for w in (0, 1):
                    ref = lined.at[self.m, half, place, s, pl.ds(w * capacity, capacity)]
                    pltpu.make_async_remote_copy(src_ref=ref, dst_ref=ref, send_sem=r_ssem.at[0, 0], recv_sem=r_rsem.at[self.m, half, place, s * 2 + w],
                                                 device_id={'ep': p.partner}, device_id_type=MESH).wait_recv()

        def load(self, i):
            half, off, place = self.where(i)
            slot = lax.rem(i, 2)
            return pltpu.make_async_copy(lined.at[self.m, half, place], line_t.at[slot], l_sem.at[slot])

        def relay(self, i, half, up):
            home = lax.rem((p.x if half else p.y) + 2, SIDE)
            step = 1 if up else SIDE - 1
            to = p.dev(step, 0) if half else p.dev(0, step)
            return pltpu.make_async_remote_copy(src_ref=sum_s.at[self.m, i, pl.ds(tokens // 2 * up, tokens // 2)], dst_ref=passing.at[self.m, half, up],
                                                send_sem=p_ssem.at[self.m, i, up], recv_sem=q_rsem.at[self.m, half, up],
                                                device_id={'ep': to}, device_id_type=MESH)

        def copy(self, i, half, up):
            step = 1 if up else SIDE - 1
            to = p.dev(step, 0) if half else p.dev(0, step)
            return pltpu.make_async_remote_copy(src_ref=sum_s.at[self.m, i], dst_ref=parts.at[self.m, half, up], send_sem=p_ssem.at[self.m, i, 0],
                                                recv_sem=p_rsem.at[self.m, half, up], device_id={'ep': to}, device_id_type=MESH)

        def sends(self, i):
            half = i % 2
            if i < 2:
                return [self.relay(i, half, up) for up in (0, 1)]
            if i < self.STEPS - 2:
                return [self.copy(i, half, 1 - (i // 2 - 1))]
            return []

        def came(self, ref, sem):
            pltpu.make_async_remote_copy(src_ref=ref, dst_ref=ref, send_sem=p_ssem.at[0, 0, 0], recv_sem=sem,
                                         device_id={'ep': p.partner}, device_id_type=MESH).wait_recv()

        def run(self):
            self.arrive(0)
            self.load(0).start()

            def step(i, c):
                @pl.when(i + 1 < self.STEPS)
                def _():
                    self.arrive(i + 1)
                    self.load(i + 1).start()
                self.load(i).wait()

                for k in range(1, self.STEPS - 1):
                    @pl.when(i == k)
                    def _():
                        for t in self.sends(k - 1):
                            t.start()

                half, off, place = self.where(i)
                home = jnp.where(half == 0, place, SIDE + place)
                slot = lax.rem(i, 2)
                total = None
                for s in range(SIDE):
                    chip = jnp.where(half == 0, p.y * SIDE + s, s * SIDE + p.x)
                    want = lax.broadcasted_iota(jnp.int32, (rows, tokens), 0) + chip * rows
                    hit = idx_all[home, self.m, 0:1, :] == want
                    for j in range(1, top_k):
                        hit = hit | (idx_all[home, self.m, j:j + 1, :] == want)
                    part = dot_tn(jnp.where(hit, 1.0, 0.0).astype(BF16), line_t[slot, s])
                    total = part if total is None else total + part
                sum_s[self.m, i] = total
                for k in range(2, self.STEPS - 2):
                    @pl.when(i == k)
                    def _():
                        up = 1 - (k // 2 - 1)
                        ref = passing.at[self.m, k % 2, up]
                        self.came(ref, q_rsem.at[self.m, k % 2, up])
                        cut = pl.ds(tokens // 2 * up, tokens // 2)
                        sum_s[self.m, k, cut] = sum_s[self.m, k, cut] + passing[self.m, k % 2, up]
                return c

            lax.fori_loop(0, self.STEPS, step, 0)

        def total(self):
            for half in (0, 1):
                acc = sum_s[self.m, self.STEPS - 2 + half]
                for up in (0, 1):
                    self.came(parts.at[self.m, half, up], p_rsem.at[self.m, half, up])
                    acc = acc + parts[self.m, half, up]
                dx_out[self.m, :, half * wide:(half + 1) * wide] = acc.astype(BF16)

        def finish(self):
            for i in range(self.STEPS):
                for t in self.sends(i):
                    t.wait_send()

    a, b = gathers
    events = {i: [] for i in range(-1, UNITS)}
    events[-1] += [lambda: a.first(0), lambda: a.first(1), lambda: a.second(0, 0), lambda: a.second(1, 0), b.begin]
    events[0] += [lambda: a.first_far(0), lambda: a.first_far(1)]
    events[1] += [lambda: a.second(0, 1), lambda: a.second(1, 1)]
    events[2] += [lambda: a.second(0, -1), lambda: a.second(1, -1)]
    events[4] += [lambda: a.second(0, 2), lambda: a.second(1, 2)]
    events[5] += [lambda: b.first(0), lambda: b.first(1)]
    events[6] += [lambda: b.second(0, 0), lambda: b.second(1, 0)]
    events[8] += [lambda: a.second_far(0)]
    events[9] += [lambda: b.first_far(0), lambda: b.first_far(1)]
    events[10] += [lambda: a.second_far(1), lambda: a.second_far(-1), lambda: a.second_far(2)]
    events[11] += [lambda: b.second(0, 1), lambda: b.second(1, 1)]
    events[12] += [lambda: b.second(0, -1), lambda: b.second(1, -1)]
    events[14] += [lambda: b.second(0, 2), lambda: b.second(1, 2)]
    for k, (ox, oy) in enumerate(ORDER):
        events[k - 1].append(functools.partial(a.from_partner, ox, oy))
    later = {1: [lambda: b.second_far(0)], 3: [lambda: b.second_far(1), lambda: b.second_far(-1)], 5: [lambda: b.second_far(2)]}

    for e in events[-1]:
        e()
    for g in (g1, g3, g2):
        g[...] = jnp.zeros_like(g)

    def recv_map(k, c):
        s = lax.rem(me + k, group)
        map_copy(s, s, k, s).wait()
        return c

    lax.fori_loop(1, group, recv_map, 0)
    own[0].wait()
    for c in weights:
        c.wait()
    units = (Units(0, ORDER), Units(1, FAR_FIRST))
    sums = (Sums(0), Sums(1))
    units[0].run(events)
    weight_grads(0, later)
    for ox, oy in ORDER:
        b.from_partner(ox, oy)
    own[1].wait()
    units[1].run({})
    for half in (0, 1):
        for o in range(1, SIDE):
            idx_wait(half, o)
    sums[0].run()
    sums[1].run()
    weight_grads(1, {})
    outs = [pltpu.make_async_copy(s, t, g_sem.at[k]) for k, (s, t) in enumerate(((g1, g1_out), (g3, g3_out), (g2, g2_out)))]
    for c in outs:
        c.start()
    for t in sums:
        t.total()

    for g in gathers:
        g.finish()
    for half in (0, 1):
        for o in range(1, SIDE):
            idx_copy(half, o).wait_send()
    for t in units + sums:
        t.finish()
    for c in outs:
        c.wait()


def START(copy):
    copy.start()


def WAIT_SEND(copy):
    copy.wait_send()


def layer_call(group, dy, topk, slots, gates, yd, x, h1, h3, w1, w3, w2):
    n_micro, tokens, d = dy.shape
    f = h1.shape[2]
    top_k = topk.shape[1]
    rows = h1.shape[1] // UNITS
    saved = h1.shape[1]
    hbm = pl.BlockSpec(memory_space=pltpu.HBM)
    vmem = pl.BlockSpec(memory_space=pltpu.VMEM)
    dma = pltpu.SemaphoreType.DMA
    shape = jax.ShapeDtypeStruct
    out = pl.pallas_call(
        functools.partial(layer_kernel, group),
        in_specs=[hbm, vmem, vmem, vmem] + [hbm] * 7,
        out_specs=[vmem, vmem] + [hbm] * 6,
        out_shape=[shape((n_micro, tokens, d), BF16), shape((n_micro, top_k, tokens), F32),
                   shape((d, f), F32), shape((d, f), F32), shape((f, d), F32),
                   shape((n_micro, group, tokens, d), BF16), shape((n_micro, UNITS, rows, d), BF16),
                   shape((n_micro, 2, SIDE, SIDE, rows, d // 2), BF16)],
        scratch_shapes=[pltpu.VMEM((group, 2 * n_micro, 1, tokens), F32), pltpu.VMEM((group, 2 * n_micro, 1, tokens), F32),
                        pltpu.VMEM((2 * SIDE, n_micro, top_k, tokens), jnp.int32),
                        pltpu.VMEM((d, f), BF16), pltpu.VMEM((d, f), BF16), pltpu.VMEM((f, d), BF16),
                        pltpu.VMEM((2, 2, tokens, d), BF16), pltpu.VMEM((2, rows, f), BF16), pltpu.VMEM((2, rows, f), BF16),
                        pltpu.VMEM((2, rows, d), BF16), pltpu.VMEM((2, 128) + yd.shape[1:], BF16), pltpu.VMEM(dy.shape, BF16),
                        pltpu.VMEM((2, 256, d), BF16), pltpu.VMEM((2, SIDE, rows, d // 2), BF16),
                        pltpu.VMEM((n_micro, 2 * SIDE, tokens, d // 2), F32), pltpu.VMEM((n_micro, 2, 2, tokens, d // 2), F32), pltpu.VMEM((n_micro, 2, 2, tokens // 2, d // 2), F32),
                        pltpu.VMEM((saved, d), BF16), pltpu.VMEM((saved, f), BF16), pltpu.VMEM((saved, f), BF16), pltpu.VMEM((saved, f), BF16),
                        pltpu.VMEM((d, f), F32), pltpu.VMEM((d, f), F32), pltpu.VMEM((f, d), F32),
                        dma((n_micro, 80)), dma((n_micro, 80)), dma((group,)), dma((group,)), dma((2 * SIDE,)), dma((2 * SIDE,)),
                        dma((n_micro, 4 * UNITS)), dma((n_micro, 2, SIDE, 2 * SIDE)), dma((n_micro, 2 * SIDE, 2)), dma((n_micro, 2, 2)), dma((n_micro, 2, 2)),
                        dma((n_micro + 1,)), dma((3,)), dma((2, 3)), dma((2,)), dma((2,)), dma((2,)), dma((2,)), dma((3,))],
        compiler_params=pltpu.CompilerParams(collective_id=0, has_side_effects=True, vmem_limit_bytes=64 * 2**20 - 2**17),
        name='layer')(dy, topk, slots, gates, yd, x, h1, h3, w1, w3, w2)
    return out[:5]


def pass_on_kernel(n, cuts, *refs):
    src, dst, held, (sem_in, sem_out) = refs[:n], refs[n:2 * n], refs[2 * n:3 * n], refs[3 * n:]
    jobs = []
    for a in range(n):
        size = src[a].shape[0] // cuts[a]
        for k in range(cuts[a]):
            at = pl.ds(k * size, size)
            jobs.append((src[a].at[at], held[a].at[at], dst[a].at[at]))
    moves = [(pltpu.make_async_copy(s, h, sem_in.at[k]), pltpu.make_async_copy(h, t, sem_out.at[k])) for k, (s, h, t) in enumerate(jobs)]
    for load, store in moves:
        load.start()
    for load, store in moves:
        load.wait()
        store.start()
    for load, store in moves:
        store.wait()


def pass_on(values, cuts):
    hbm = pl.BlockSpec(memory_space=pltpu.HBM)
    n = len(values)
    jobs = sum(cuts)
    return pl.pallas_call(
        functools.partial(pass_on_kernel, n, cuts),
        in_specs=[hbm] * n, out_specs=[hbm] * n,
        out_shape=[jax.ShapeDtypeStruct(v.shape, v.dtype) for v in values],
        scratch_shapes=[pltpu.VMEM(v.shape, v.dtype) for v in values] + [pltpu.SemaphoreType.DMA((jobs,)), pltpu.SemaphoreType.DMA((jobs,))],
        compiler_params=pltpu.CompilerParams(vmem_limit_bytes=64 * 2**20 - 2**17),
        name='pass_on')(*values)


def solution(mesh):
    group = mesh.shape['ep']
    tok_spec = P(None, ('dp', 'ep'))
    w_spec = P('ep')
    grad_w_spec = P(('dp', 'ep'))

    def local_step(grad_out, expert_out, gate_vals, topk_idx, slot_idx, x_dispatch, h1_pre, h3_pre, w_gate, w_up, w_down):
        n_micro, tokens, top_k, d = expert_out.shape
        turned = [jnp.swapaxes(v, 1, 2) for v in (topk_idx, slot_idx, gate_vals)]
        dx, dg, g1, g3, g2 = layer_call(
            group, grad_out, *turned, expert_out.reshape(n_micro * tokens, top_k, d),
            x_dispatch[:, 0], h1_pre[:, 0], h3_pre[:, 0], w_gate[0], w_up[0], w_down[0])
        dx, dg, g1, g3, g2 = pass_on((dx, dg, g1, g3, g2), (n_micro, 1, 4, 4, 4))
        return dx, jnp.swapaxes(dg, 1, 2), g1[None], g3[None], g2[None]

    in_specs = (tok_spec, tok_spec, tok_spec, tok_spec, tok_spec, tok_spec, tok_spec, tok_spec, w_spec, w_spec, w_spec)
    out_specs = (tok_spec, tok_spec, grad_w_spec, grad_w_spec, grad_w_spec)
    return jax.shard_map(local_step, mesh=mesh, in_specs=in_specs, out_specs=out_specs, check_vma=False)
```
